512 devices in a mesh: member: 2 (over y), blk: 256 (over z, x, core).
Axes of the slice: x: 8, y: 2, z: 16, core: 2. Of those that a mesh axis runs over, the one named last changes fastest.
The devices are a block of a 8x8x16 slice.
Arguments:
- pressure: float32 [55, 131072], P(None, ('member', 'blk')), parts along dimension 1, may hold values from -6 to 6
- velocity: float32 [55, 393216], P(None, ('member', 'blk')), parts along dimension 1, may hold values from -3 to 3
- tracers: float32 [3, 55, 131072], P(None, None, ('member', 'blk')), parts along dimension 2, may hold values from 0.1 to 2
- tendency: float32 [55, 131072], P(None, ('member', 'blk')), parts along dimension 1, may hold values from -6 to 6
- pattern: float32 [131072], P(('member', 'blk')), parts along dimension 0, may hold values from -0.9 to 0.9
- coupling: float32 [55, 65536], P(None, 'blk'), may hold values from 0.3 to 3
- edge_length: float32 [196608], P('blk'), may hold values from 0.7 to 1.4
- inv_distance: float32 [196608], P('blk'), may hold values from 0.7 to 1.4
- inv_area: float32 [65536], P('blk'), may hold values from 0.7 to 1.4
- edge_ends: int32 [2, 196608], P(None, 'blk'), may hold values from 0 to 351, as said below
- halo_ends: int32 [2, 32768], P(None, 'blk'), may hold values from 0 to 351, as said below
- cell_edges: int32 [8, 65536], P(None, 'blk'), may hold values from 0 to 895, as said below
- cell_signs: int32 [8, 65536], P(None, 'blk'), may hold values from -1 to 1, as said below
- cell_send: int32 [6, 4096], P(None, 'blk'), may hold values from 0 to 255, as said below
- edge_send: int32 [4, 8192], P(None, 'blk'), may hold values from 0 to 767, as said below
Outputs:
- new_pressure: float32 [55, 131072], P(None, ('member', 'blk')), parts along dimension 1
- new_velocity: float32 [55, 393216], P(None, ('member', 'blk')), parts along dimension 1
- new_tracers: float32 [3, 55, 131072], P(None, None, ('member', 'blk')), parts along dimension 2
The draws below stay inside these ranges and needn't reach their ends.
There are 2 independent parts, one for each index of `member`. The reference program is written for one: setup_inputs(seed, part) draws one part's arguments, and reference() takes and returns one part's arrays. A program takes and returns all parts, laid end to end along the dimension named above; an argument that names none is the same for every part. Nothing has to cross between parts.
Inputs may be any that keep to these rules, and one draw needn't show every extreme that they name: `cell_send`: the cells form a periodic hexagonal lattice; each device holds a 16 x 16 patch, numbered in a drawn order; a patch touches the patches of the devices at index offsets 1, -1, 16, -16, 15 and 1 - 16 (modulo 256). Row k of a device's block lists the own cells that the device at index + o_k receives, o = (1, -1, 16, -16, 15, 1 - 16); rows 0 to 3 hold 16 live entries, rows 4 and 5 one live entry first, the rest repeat it. `edge_send`: row k of a device's block lists the own edges that the device at index + p_k receives, p = (1, 16, -16, 1 - 16); the live entries come first, 31, 16, 15 and 1 of them, the rest repeat a live one. `edge_ends`: row 0 is an own cell; row 1 is the neighbouring cell, own or received; the numbering is consistent with cell_send. `halo_ends`: for live received slots, the owner's edge's start and end as the receiver numbers them; other slots hold cells that no output reads. `cell_edges`: each own cell lists its six edges once each, in a drawn order, and two unused entries, whose sign is 0. `cell_signs`: 1 where the cell is the edge's start, -1 where it is its end, 0 on the unused entries.
All inputs are finite; a program needn't handle non-finite values.
Results may differ from the reference program's by a relative error of at most 0.0003.
Values sent between devices are 32-bit elements; how exact they have to be, the bound alone decides.
No kernel may reach another device: no remote copies, remote signals or barrier semaphores. Data moves between devices by JAX's collectives and lax.ppermute only.
A program may use at most 128 MiB of HBM per device.

```python
import math
import jax
import jax.numpy as jnp
import numpy as np

B = 16
L = 55
NT = 3
SUBSTEPS = 6
BROW = 16
ALL_CELLS = 65536
ALL_EDGES = 196608
N_BLK = 256


def neighbour(across, upward, shift_a, shift_b):
    moved_a = across + shift_a
    moved_b = upward + shift_b
    block_a = np.where(moved_a >= B, 1, np.where(moved_a < 0, -1, 0))
    block_b = np.where(moved_b >= B, 1, np.where(moved_b < 0, -1, 0))
    return (block_a, block_b, moved_a - block_a * B, moved_b - block_b * B)


def cell_slot(block_a, block_b, moved_a, moved_b):
    peer_row = np.where((block_a == -1) & (block_b == 0), 0, np.where((block_a == 1) & (block_b == 0), 1, np.where((block_a == 0) & (block_b == -1), 2, np.where((block_a == 0) & (block_b == 1), 3, np.where((block_a == 1) & (block_b == -1), 4, 5)))))
    within = np.where(peer_row < 2, moved_b, np.where(peer_row < 4, moved_a, 0))
    return B * B + peer_row * B + within


def static_layout():
    own_cells = B * B
    own_edges = 3 * B * B
    lattice = np.arange(own_cells)
    across = lattice % B
    upward = lattice // B
    steps_a = (1, 0, 1)
    steps_b = (0, 1, -1)
    end_inside = []
    end_lattice = []
    end_slot = []
    slot_inside = []
    slot_lattice = []
    slot_index = []
    slot_sign = []
    for direction in range(3):
        block_a, block_b, moved_a, moved_b = neighbour(across, upward, steps_a[direction], steps_b[direction])
        inside = (block_a == 0) & (block_b == 0)
        end_inside.append(inside)
        end_lattice.append(moved_a + B * moved_b)
        end_slot.append(cell_slot(block_a, block_b, moved_a, moved_b))
        slot_inside.append(np.ones(own_cells, bool))
        slot_lattice.append(direction * own_cells + lattice)
        slot_index.append(np.zeros(own_cells, np.int64))
        slot_sign.append(np.ones(own_cells, np.int64))
    for direction in range(3):
        block_a, block_b, moved_a, moved_b = neighbour(across, upward, -steps_a[direction], -steps_b[direction])
        inside = (block_a == 0) & (block_b == 0)
        peer_row = np.where((block_a == -1) & (block_b == 0), 0, np.where((block_a == 0) & (block_b == -1), 1, np.where((block_a == 0) & (block_b == 1), 2, 3)))
        if direction == 0:
            first_within = moved_b
        else:
            first_within = B + moved_b - 1
        within = np.where(peer_row == 0, first_within, np.where(peer_row < 3, moved_a, 0))
        slot_inside.append(inside)
        slot_lattice.append(direction * own_cells + moved_a + B * moved_b)
        slot_index.append(own_edges + peer_row * 2 * B + within)
        slot_sign.append(-np.ones(own_cells, np.int64))
    for padding in range(2):
        slot_inside.append(np.ones(own_cells, bool))
        slot_lattice.append(np.zeros(own_cells, np.int64))
        slot_index.append(np.zeros(own_cells, np.int64))
        slot_sign.append(np.zeros(own_cells, np.int64))
    within = np.arange(B)
    cell_rows = np.stack([B - 1 + B * within, B * within, within + B * (B - 1), within, np.full(B, B * (B - 1)), np.full(B, B - 1)])
    double = np.arange(2 * B)
    row_zero = np.where(double < B, B - 1 + B * np.minimum(double, B - 1), np.where(double < 2 * B - 1, 2 * own_cells + B - 1 + B * np.clip(double - B + 1, 0, B - 1), B - 1))
    row_one = np.where(double < B, own_cells + np.minimum(double, B - 1) + B * (B - 1), own_cells + B * (B - 1))
    row_two = np.where(double < B - 1, 2 * own_cells + np.minimum(double, B - 1), 2 * own_cells)
    row_three = np.full(2 * B, 2 * own_cells + B - 1)
    edge_rows = np.stack([row_zero, row_one, row_two, row_three])
    start_zero = np.where(double < B, own_cells + double, np.where(double < 2 * B - 1, own_cells + double - B + 1, 0))
    end_zero = np.where(double < B, B * double, np.where(double < 2 * B - 1, B * (double - B), 0))
    start_one = np.where(double < B, own_cells + 2 * B + double, 0)
    end_one = np.where(double < B, double, 0)
    start_two = np.where(double < B - 1, own_cells + 3 * B + double, 0)
    end_two = np.where(double < B - 1, double + 1 + B * (B - 1), 0)
    start_three = np.where(double < 1, own_cells + 5 * B, 0)
    end_three = np.where(double < 1, B * (B - 1), 0)
    halo_start = np.concatenate([start_zero, start_one, start_two, start_three])
    halo_end = np.concatenate([end_zero, end_one, end_two, end_three])
    return (np.concatenate(end_inside), np.concatenate(end_lattice).astype(np.int32), np.concatenate(end_slot).astype(np.int32), np.stack(slot_inside, axis=1), np.stack(slot_lattice, axis=1).astype(np.int32), np.stack(slot_index, axis=1).astype(np.int32), np.stack(slot_sign, axis=1).astype(np.int32), cell_rows.astype(np.int32), edge_rows.astype(np.int32), halo_start.astype(np.int32), halo_end.astype(np.int32))


def lattice_tables(key):
    own_cells = B * B
    own_edges = 3 * B * B
    end_inside, end_lattice, end_slot, slot_inside, slot_lattice, slot_index, slot_sign, cell_rows, edge_rows, halo_start, halo_end = static_layout()
    cell_order = jax.vmap(lambda single: jax.random.permutation(single, own_cells))(jax.random.split(jax.random.fold_in(key, 101), N_BLK)).astype(jnp.int32)
    edge_order = jax.vmap(lambda single: jax.random.permutation(single, own_edges))(jax.random.split(jax.random.fold_in(key, 102), N_BLK)).astype(jnp.int32)
    device = jnp.arange(N_BLK, dtype=jnp.int32)[:, None]
    start_local = cell_order[:, (np.arange(own_edges) % own_cells).astype(np.int32)]
    end_local = jnp.where(end_inside[None, :], cell_order[:, end_lattice], end_slot[None, :])
    ends_table = jnp.zeros((2, N_BLK, own_edges), jnp.int32).at[:, device, edge_order].set(jnp.stack([start_local, end_local]))
    edge_ends = ends_table.reshape(2, N_BLK * own_edges)
    halo_starts = jnp.broadcast_to(jnp.asarray(halo_start)[None, :], (N_BLK, 8 * B))
    halo_finish = cell_order[:, halo_end]
    halo_ends = jnp.stack([halo_starts, halo_finish]).reshape(2, N_BLK * 8 * B)
    slot_value = jnp.where(slot_inside[None], edge_order[:, slot_lattice], slot_index[None])
    sign_table = jnp.broadcast_to(jnp.asarray(slot_sign)[None], (N_BLK, own_cells, 8))
    scores = jax.random.randint(jax.random.fold_in(key, 103), (N_BLK, own_cells, 8), 0, 1 << 20) * 8 + jnp.arange(8, dtype=jnp.int32)
    shuffle = jnp.argsort(scores, axis=-1)
    slot_value = jnp.take_along_axis(slot_value, shuffle, axis=-1)
    sign_table = jnp.take_along_axis(sign_table, shuffle, axis=-1)
    placed = jnp.zeros((N_BLK, own_cells, 8), jnp.int32).at[device, cell_order].set(slot_value)
    placed_signs = jnp.zeros((N_BLK, own_cells, 8), jnp.int32).at[device, cell_order].set(sign_table)
    cell_edges = placed.transpose(2, 0, 1).reshape(8, N_BLK * own_cells)
    cell_signs = placed_signs.transpose(2, 0, 1).reshape(8, N_BLK * own_cells)
    cell_send = cell_order[:, cell_rows].transpose(1, 0, 2).reshape(6, N_BLK * B)
    edge_send = edge_order[:, edge_rows].transpose(1, 0, 2).reshape(4, N_BLK * 2 * B)
    return (edge_ends, halo_ends, cell_edges, cell_signs, cell_send, edge_send)


def draw_edge_ends(key, part):
    return lattice_tables(key)[0]


def draw_halo_ends(key, part):
    return lattice_tables(key)[1]


def draw_cell_edges(key, part):
    return lattice_tables(key)[2]


def draw_cell_signs(key, part):
    return lattice_tables(key)[3]


def draw_cell_send(key, part):
    return lattice_tables(key)[4]


def draw_edge_send(key, part):
    return lattice_tables(key)[5]


def shard_levels(stream_key, extent, cuts, least, top_value):
    def one(dim, blocks):
        steps = jax.random.uniform(jax.random.fold_in(jax.random.fold_in(stream_key, 6), dim), (blocks,), jnp.float32, least / len(cuts), top_value / len(cuts))
        return jnp.repeat(jnp.exp(steps), extent[dim] // blocks).reshape((-1,) + (1,) * (len(extent) - dim - 1))

    loudness = one(*cuts[0])
    for cut in cuts[1:]:
        loudness = loudness * one(*cut)
    return loudness


def scatter_about(stream_key, shape, scale, most, cuts=(), held_as=jnp.bfloat16):
    factor_of = shard_levels(stream_key, shape, cuts, -0.22, 0.18) if cuts else 1.0
    values = jax.random.normal(stream_key, shape, jnp.float32) * scale * factor_of
    return jnp.minimum(jnp.maximum(values, -most), most).astype(held_as)


def setup_inputs(seed: int = 0, part: int = 0) -> dict:
    seeds = jax.random.split(jax.random.key(seed), 16)
    own_keys = jax.random.split(jax.random.fold_in(seeds[15], part), 16)
    pressure = scatter_about(own_keys[0], (L, ALL_CELLS), 1.0, 6.0, ((1, 256),), jnp.float32)
    velocity = scatter_about(own_keys[1], (L, ALL_EDGES), 0.5, 3.0, ((1, 256),), jnp.float32)
    tracers = jnp.clip(jnp.exp(math.log(2.0) - 2.9957323 * jax.random.uniform(own_keys[2], (NT, L, ALL_CELLS), jnp.float32) ** shard_levels(own_keys[2], (NT, L, ALL_CELLS), ((2, 256),), -0.2, 0.2)), 0.1, 2.0)
    tendency = scatter_about(own_keys[3], (L, ALL_CELLS), 1.0, 6.0, ((1, 256),), jnp.float32)
    pattern = jnp.clip(jax.random.uniform(own_keys[4], (ALL_CELLS,), jnp.float32, -0.9, 0.9) * shard_levels(own_keys[4], (ALL_CELLS,), ((0, 256),), -0.4, 0.0), -0.9, 0.9)
    coupling = jnp.clip(jnp.exp(math.log(3.0) - 2.3025851 * jax.random.uniform(seeds[5], (L, ALL_CELLS), jnp.float32) ** shard_levels(seeds[5], (L, ALL_CELLS), ((1, 256),), -0.2, 0.2)), 0.3, 3.0)
    edge_length = jnp.clip(jnp.exp(math.log(1.4) - 0.6931472 * jax.random.uniform(seeds[6], (ALL_EDGES,), jnp.float32) ** shard_levels(seeds[6], (ALL_EDGES,), ((0, 256),), -0.2, 0.2)), 0.7, 1.4)
    inv_distance = jnp.clip(jnp.exp(math.log(1.4) - 0.6931472 * jax.random.uniform(seeds[7], (ALL_EDGES,), jnp.float32) ** shard_levels(seeds[7], (ALL_EDGES,), ((0, 256),), -0.2, 0.2)), 0.7, 1.4)
    inv_area = jnp.clip(jnp.exp(math.log(1.4) - 0.6931472 * jax.random.uniform(seeds[8], (ALL_CELLS,), jnp.float32) ** shard_levels(seeds[8], (ALL_CELLS,), ((0, 256),), -0.2, 0.2)), 0.7, 1.4)
    edge_ends = draw_edge_ends(jax.random.fold_in(seeds[15], 71), part)
    halo_ends = draw_halo_ends(jax.random.fold_in(seeds[15], 71), part)
    cell_edges = draw_cell_edges(jax.random.fold_in(seeds[15], 71), part)
    cell_signs = draw_cell_signs(jax.random.fold_in(seeds[15], 71), part)
    cell_send = draw_cell_send(jax.random.fold_in(seeds[15], 71), part)
    edge_send = draw_edge_send(jax.random.fold_in(seeds[15], 71), part)
    return dict(pressure=pressure, velocity=velocity, tracers=tracers, tendency=tendency, pattern=pattern, coupling=coupling, edge_length=edge_length, inv_distance=inv_distance, inv_area=inv_area, edge_ends=edge_ends, halo_ends=halo_ends, cell_edges=cell_edges, cell_signs=cell_signs, cell_send=cell_send, edge_send=edge_send)


grad_scale = 0.25
spread_scale = 0.25
force_scale = 0.5
tracer_scale = 0.05


def vertical_taper(levels):
    height = jnp.arange(levels, dtype=jnp.float32)
    return jnp.minimum(1.0, (levels - 1.0 - height) / (0.25 * levels))


def factor_columns(coupling):
    levels = coupling.shape[0]
    upper_link = jnp.concatenate([coupling[1:], jnp.zeros_like(coupling[:1])], axis=0)
    diagonal = 1.0 + coupling + upper_link
    inverses = []
    ratios = []
    for height in range(levels):
        if height == 0:
            divisor = diagonal[0]
        else:
            divisor = diagonal[height] + coupling[height] * ratios[-1]
        inverse = 1.0 / divisor
        inverses.append(inverse)
        ratios.append(-upper_link[height] * inverse)
    return jnp.stack(inverses), jnp.stack(ratios)


def solve_columns(source, coupling, inverses, ratios):
    levels = source.shape[0]
    forward = [source[0] * inverses[0]]
    for height in range(1, levels):
        forward.append((source[height] + coupling[height] * forward[-1]) * inverses[height])
    result = [forward[-1]]
    for height in range(levels - 2, -1, -1):
        result.append(forward[height] - ratios[height] * result[-1])
    return jnp.stack(result[::-1])


def extended_maps(cell_send, edge_send):
    own_cells = B * B
    own_edges = 3 * B * B
    cell_offsets = jnp.array([1, -1, BROW, -BROW, BROW - 1, 1 - BROW], dtype=jnp.int32)
    edge_offsets = jnp.array([1, BROW, -BROW, 1 - BROW], dtype=jnp.int32)
    device = jnp.arange(N_BLK, dtype=jnp.int32)[:, None]
    position = jnp.arange(own_cells + 6 * B, dtype=jnp.int32)[None, :]
    peer_row = jnp.clip((position - own_cells) // B, 0, 5)
    within = (position - own_cells) % B
    source = (device - cell_offsets[peer_row]) % N_BLK
    remote = source * own_cells + cell_send[peer_row, source * B + within]
    cell_map = jnp.where(position < own_cells, device * own_cells + position, remote)
    position = jnp.arange(own_edges + 8 * B, dtype=jnp.int32)[None, :]
    peer_row = jnp.clip((position - own_edges) // (2 * B), 0, 3)
    within = (position - own_edges) % (2 * B)
    source = (device - edge_offsets[peer_row]) % N_BLK
    remote = source * own_edges + edge_send[peer_row, source * (2 * B) + within]
    edge_map = jnp.where(position < own_edges, device * own_edges + position, remote)
    return cell_map.astype(jnp.int32), edge_map.astype(jnp.int32)


def reference(pressure, velocity, tracers, tendency, pattern, coupling, edge_length, inv_distance, inv_area, edge_ends, halo_ends, cell_edges, cell_signs, cell_send, edge_send):
    own_cells = B * B
    own_edges = 3 * B * B
    cell_map, edge_map = extended_maps(cell_send, edge_send)
    local_ends = edge_ends.reshape(2, N_BLK, own_edges)
    start_global = jnp.take_along_axis(cell_map, local_ends[0], axis=1).reshape(-1)
    end_global = jnp.take_along_axis(cell_map, local_ends[1], axis=1).reshape(-1)
    all_ends = jnp.concatenate([local_ends, halo_ends.reshape(2, N_BLK, 8 * B)], axis=2)
    slot_edges = cell_edges.reshape(8, N_BLK, own_cells)
    edge_global = []
    first_global = []
    last_global = []
    weights = []
    for column_slot in range(8):
        chosen = slot_edges[column_slot]
        edge_global.append(jnp.take_along_axis(edge_map, chosen, axis=1).reshape(-1))
        first_global.append(jnp.take_along_axis(cell_map, jnp.take_along_axis(all_ends[0], chosen, axis=1), axis=1).reshape(-1))
        last_global.append(jnp.take_along_axis(cell_map, jnp.take_along_axis(all_ends[1], chosen, axis=1), axis=1).reshape(-1))
        weights.append(cell_signs[column_slot].astype(jnp.float32) * edge_length[edge_global[-1]] * inv_area)
    forcing = force_scale * (1.0 + pattern[None, :] * vertical_taper(L)[:, None]) * tendency
    inverses, ratios = factor_columns(coupling)
    current = pressure
    edge_flow = velocity
    flow_total = jnp.zeros_like(velocity)
    for substep in range(SUBSTEPS):
        edge_flow = edge_flow - grad_scale * inv_distance * (current[:, end_global] - current[:, start_global])
        flow_total = flow_total + edge_flow
        spread = weights[0] * edge_flow[:, edge_global[0]]
        for column_slot in range(1, 8):
            spread = spread + weights[column_slot] * edge_flow[:, edge_global[column_slot]]
        current = solve_columns(current - spread_scale * spread + forcing, coupling, inverses, ratios)
    mean_flow = flow_total * (1.0 / SUBSTEPS)
    tracer_spread = jnp.zeros_like(tracers)
    for column_slot in range(8):
        chosen_flow = mean_flow[:, edge_global[column_slot]]
        tracer_flux = jnp.maximum(chosen_flow, 0.0)[None] * tracers[:, :, first_global[column_slot]] + jnp.minimum(chosen_flow, 0.0)[None] * tracers[:, :, last_global[column_slot]]
        tracer_spread = tracer_spread + weights[column_slot] * tracer_flux
    new_tracers = tracers - tracer_scale * tracer_spread
    return current, edge_flow, new_tracers
```

```python
import functools

import jax
import jax.numpy as jnp
from jax import lax
from jax.experimental import pallas as pl
from jax.experimental.pallas import tpu as pltpu
from jax.sharding import PartitionSpec as P

SUBSTEPS = 6
grad_scale = 0.25
spread_scale = 0.25
force_scale = 0.5
tracer_scale = 0.05

SIDE = 16
CELLS = SIDE * SIDE
DEPTH = SUBSTEPS
COL = 32
PAD_A = 8
GROUP = 56
F32 = jnp.float32
BF16 = jnp.bfloat16
I32 = jnp.int32


def iota(shape, dim):
    return lax.broadcasted_iota(I32, shape, dim)


def one_hot(row, count):
    return jnp.where(iota((count, row.shape[1]), 0) == row, 1.0, 0.0).astype(BF16)


def halves(x):
    hi = x.astype(BF16)
    return hi, (x - hi.astype(F32)).astype(BF16)


def dot(x, y):
    return lax.dot_general(x, y, (((1,), (0,)), ((), ())), preferred_element_type=F32)


def dot_t(x, y):
    return lax.dot_general(x, y, (((1,), (1,)), ((), ())), preferred_element_type=F32)


def pick(x, table):
    hi, lo = halves(x)
    return dot(hi, table) + dot(lo, table)


def pick_t(x, table):
    hi, lo = halves(x)
    return dot_t(hi, table) + dot_t(lo, table)


def rows8(*rows):
    width = rows[0].shape[1]
    at = iota((8, width), 0)
    out = jnp.zeros((8, width), F32)
    for number, row in enumerate(rows):
        out = jnp.where(at == number, row, out)
    return out


def sixth(j):
    return (j * 43) >> 8


def prepare(
    send_ref, p_ref, vel_ref, trc_ref, tend_ref, pat_ref, coup_ref, len_ref, invd_ref, ia_ref, ends_ref,
    own_ref, trcl_ref, up_ref, dn_ref, east_ref, west_ref, meta_ref,
    x_ref, v_ref,
):
    levels = p_ref.shape[0]
    edges = vel_ref.shape[1]
    start = ends_ref[0:1, :]
    end = ends_ref[1:2, :]
    start_hot = one_hot(start, CELLS)
    end_hot = one_hot(end, CELLS)
    adjacent = dot_t(
        jnp.concatenate([start_hot, end_hot], axis=1), jnp.concatenate([end_hot, start_hot], axis=1)
    ).astype(BF16)
    cell = iota((1, CELLS), 1)
    seeds = []
    for side in (1, 0, 3, 2):
        hit = cell == send_ref[side, 0]
        for s in range(1, SIDE):
            hit = hit | (cell == send_ref[side, s])
        seeds.append(jnp.where(hit, 1.0, 0.0))
    reached = rows8(*seeds)
    far = 1.0 - reached
    for _ in range(SIDE // 2 - 1):
        reached = jnp.minimum(1.0, reached + dot(reached.astype(BF16), adjacent))
        far = far + (1.0 - reached)
    half = SIDE // 2
    a = jnp.where(far[0:1] < half, far[0:1], SIDE - 1.0 - far[1:2])
    b = jnp.where(far[2:3] < half, far[2:3], SIDE - 1.0 - far[3:4])
    place = (a * SIDE + b).astype(I32)
    corners = rows8(a, b).astype(BF16)
    at_start = dot(corners, start_hot)
    at_end = dot(corners, end_hot)
    a_s, b_s = at_start[0:1], at_start[1:2]
    a_e, b_e = at_end[0:1], at_end[1:2]
    rim_hot = one_hot(end - CELLS, 6 * SIDE)
    met = dot_t(rows8(b_s, jnp.ones_like(b_s)).astype(BF16), rim_hot)
    rim_b = jnp.where(met[1:2] > 1.5, (met[0:1] - 1.0) * 0.5, met[0:1])
    rim_b = dot(rows8(rim_b).astype(BF16), rim_hot)[0:1]
    outside = end >= CELLS
    peer = (end - CELLS) >> 4
    zero = jnp.zeros_like(end)
    direction_out = jnp.where(
        peer == 3, zero + 1, jnp.where(peer == 1, jnp.where(jnp.abs(b_s - rim_b) < 0.5, zero, zero + 2), zero + 2)
    )
    da = a_e - a_s
    db = b_e - b_s
    direction_in = jnp.where(jnp.abs(db) < 0.5, zero, jnp.where(jnp.abs(da) < 0.5, zero + 1, zero + 2))
    onward = outside | (da > 0.5) | ((jnp.abs(da) < 0.5) & (db > 0.5))
    direction = jnp.where(outside, direction_out, direction_in)
    sense = jnp.where(onward, 1.0, -1.0)
    anchor = jnp.where(onward, a_s * SIDE + b_s, a_e * SIDE + b_e).astype(I32)
    spot = direction * CELLS + anchor
    at8 = iota((8, edges), 0)
    meta = jnp.where(at8 == 0, spot, jnp.where(at8 == 1, sense.astype(I32), zero))
    meta_ref[...] = meta
    meta_ref[2:3, 0:CELLS] = place
    x_ref[...] = jnp.zeros(x_ref.shape, F32)
    height = iota((levels, 1), 0).astype(F32)
    taper = jnp.minimum(1.0, (levels - 1.0 - height) / (0.25 * levels))
    x_ref[0:levels] = p_ref[...]
    x_ref[GROUP : GROUP + levels] = force_scale * (1.0 + pat_ref[...] * taper) * tend_ref[...]
    x_ref[2 * GROUP : 2 * GROUP + levels] = coup_ref[...]
    x_ref[3 * GROUP : 3 * GROUP + 1] = ia_ref[...]
    first = 3 * GROUP + 8
    for n in range(trc_ref.shape[0]):
        x_ref[first + n * GROUP : first + n * GROUP + levels] = trc_ref[n]
    place_hot = one_hot(place, CELLS)
    moved = pick_t(x_ref[...], place_hot)
    own_ref[0 : 3 * GROUP] = moved[0 : 3 * GROUP]
    trcl_ref[...] = moved[first:]
    v_ref[...] = jnp.zeros(v_ref.shape, F32)
    v_ref[0:levels] = vel_ref[...] * sense
    v_ref[GROUP : GROUP + 1] = len_ref[...]
    v_ref[GROUP + 1 : GROUP + 2] = invd_ref[...]
    v_hi, v_lo = halves(v_ref[...])
    lengths, distances = [], []
    for k in range(3):
        spot_hot = one_hot(spot - k * CELLS, CELLS)
        got = dot_t(v_hi, spot_hot) + dot_t(v_lo, spot_hot)
        own_ref[(3 + k) * GROUP : (4 + k) * GROUP] = got[0:GROUP]
        lengths.append(got[GROUP : GROUP + 1])
        distances.append(got[GROUP + 1 : GROUP + 2])
    own_ref[6 * GROUP : 6 * GROUP + 8] = rows8(*lengths, *distances, moved[3 * GROUP : 3 * GROUP + 1])
    column = iota((1, 512), 1)
    part = column >> 7
    j = column & 127
    sa = sixth(j)
    sb = j - sa * 6
    strip = jnp.where(
        part == 0, sa * SIDE + SIDE - DEPTH + sb,
        jnp.where(part == 1, sa * SIDE + sb, jnp.where(part == 2, j + CELLS - DEPTH * SIDE, j)),
    )
    strip = jnp.where(j < DEPTH * SIDE, strip, -1)
    t = j - DEPTH * SIDE
    rim = jnp.where(
        part == 0, t * SIDE + SIDE - 1, jnp.where(part == 1, t * SIDE, jnp.where(part == 2, t + CELLS - SIDE, t))
    )
    rim = jnp.where((t >= 0) & (t < SIDE), rim, -1)
    strips = pick(own_ref[...], one_hot(strip, CELLS))
    rims = pick(trcl_ref[...], one_hot(rim, CELLS))
    top = strips[0 : rims.shape[0]] + rims
    rest = strips[rims.shape[0] :]
    for number, ref in enumerate((up_ref, dn_ref, east_ref, west_ref)):
        ref[0 : rims.shape[0]] = top[:, 128 * number : 128 * number + 128]
        ref[rims.shape[0] :] = rest[:, 128 * number : 128 * number + 128]


def advance(
    own_ref, trcl_ref, south_ref, north_ref, west_ref, east_ref, meta_ref, vel_ref, invd_ref,
    newp_ref, newv_ref, newt_ref,
    big_ref, trc_ref, hist_ref, t_ref, f_ref, inv_ref, al_ref, be_ref, out_ref, dq_ref,
):
    levels = newp_ref.shape[0]
    species = newt_ref.shape[0]
    edges = newv_ref.shape[1]
    rows = own_ref.shape[0]
    trows = trcl_ref.shape[0]
    q = iota((1, 512), 1)
    qa = q >> 5
    qb = (q & 31) - DEPTH
    inside = (qb >= 0) & (qb < SIDE)
    below = (qb >= -DEPTH) & (qb < 0)
    above = (qb >= SIDE) & (qb < SIDE + DEPTH)
    src = jnp.where(
        inside, qa * SIDE + qb,
        jnp.where(below, 256 + qa * DEPTH + qb + DEPTH, jnp.where(above, 384 + qa * DEPTH + qb - SIDE, -1)),
    )
    tsrc = jnp.where(
        inside, qa * SIDE + qb, jnp.where(qb == -1, 256 + 96 + qa, jnp.where(qb == SIDE, 384 + 96 + qa, -1))
    )
    s_val, n_val = south_ref[...], north_ref[...]
    core = pick(jnp.concatenate([own_ref[...], s_val, n_val], axis=1), one_hot(src, 512))
    tcore = pick(
        jnp.concatenate([trcl_ref[...], s_val[0:trows], n_val[0:trows]], axis=1), one_hot(tsrc, 512)
    )
    for s in range(4):
        big_ref[pl.ds(2 + s, rows, stride=8), :] = core[:, 128 * s : 128 * s + 128]
        trc_ref[pl.ds(2 + s, trows, stride=8), :] = tcore[:, 128 * s : 128 * s + 128]
    q = iota((1, 256), 1)
    qb = (q & 31) - DEPTH
    inside = (qb >= 0) & (qb < SIDE)
    below = (qb >= -DEPTH) & (qb < 0)
    above = (qb >= SIDE) & (qb < SIDE + DEPTH)
    for side, ref in ((0, west_ref), (6, east_ref)):
        qa = (q >> 5) - (PAD_A - DEPTH if side == 0 else 0)
        src = jnp.where(
            inside, qa * SIDE + qb,
            jnp.where(below, 112 + qa * DEPTH + qb + DEPTH, jnp.where(above, 148 + qa * DEPTH + qb - SIDE, -1)),
        )
        src = jnp.where((qa >= 0) & (qa < DEPTH), src, -1)
        near = DEPTH - 1 if side == 0 else 0
        tsrc = jnp.where(
            inside, 96 + qb, jnp.where(qb == -1, 184, jnp.where(qb == SIDE, 185, -1))
        )
        tsrc = jnp.where(qa == near, tsrc, -1)
        hi, lo = halves(ref[...])
        hot = one_hot(src, 256)
        thot = one_hot(tsrc, 256)
        flank = dot(hi, hot) + dot(lo, hot)
        tflank = dot(hi[0:trows], thot) + dot(lo[0:trows], thot)
        for s in range(2):
            big_ref[pl.ds(side + s, rows, stride=8), :] = flank[:, 128 * s : 128 * s + 128]
            trc_ref[pl.ds(side + s, trows, stride=8), :] = tflank[:, 128 * s : 128 * s + 128]

    lane = iota((8, 128), 1)
    first_group = lane < COL
    last_group = lane >= 128 - COL

    def b_up(x):
        return pltpu.roll(x, 127, 1)

    def b_dn(x):
        return pltpu.roll(x, 1, 1)

    def a_up(x):
        y = pltpu.roll(x, 128 - COL, 1)
        return jnp.where(last_group, pltpu.roll(y, 7, 0), y)

    def a_dn(x):
        y = pltpu.roll(x, COL, 1)
        return jnp.where(first_group, pltpu.roll(y, 1, 0), y)

    def ups(x):
        right = a_up(x)
        return right, b_up(x), b_dn(right)

    def back(x0, x1, x2):
        return a_dn(x0), b_dn(x1), b_up(a_dn(x2))

    def row(ref, number):
        return ref[8 * number : 8 * number + 8, :]

    def dyn(ref, number):
        return ref[pl.ds(pl.multiple_of(8 * number, 8), 8), :]

    length = [row(big_ref, 6 * GROUP + k) for k in range(3)]
    grad = [grad_scale * row(big_ref, 6 * GROUP + 3 + k) for k in range(3)]
    area = row(big_ref, 6 * GROUP + 6)
    pull = spread_scale * area
    out_coef = [length[k] * grad[k] for k in range(3)]
    in_coef = back(*out_coef)
    out_coef = [pull * c for c in out_coef]
    in_coef = [pull * c for c in in_coef]
    mid_coef = -(out_coef[0] + out_coef[1] + out_coef[2] + in_coef[0] + in_coef[1] + in_coef[2])

    def first_spread(l, carry):
        w = [length[k] * dyn(big_ref, (3 + k) * GROUP + l) for k in range(3)]
        w_in = back(*w)
        total = (w[0] - w_in[0]) + (w[1] - w_in[1]) + (w[2] - w_in[2])
        at = pl.ds(pl.multiple_of(8 * l, 8), 8)
        t_ref[at, :] = dyn(big_ref, GROUP + l) - pull * total
        hist_ref[at, :] = dyn(big_ref, l)
        return carry

    lax.fori_loop(0, levels, first_spread, 0, unroll=5)

    middle = levels // 2
    c = [row(big_ref, 2 * GROUP + l) for l in range(levels)] + [jnp.zeros((8, 128), F32)]
    diag = [1.0 + c[l] + c[l + 1] for l in range(levels)]
    inverse = [None] * levels
    older, old = None, jnp.ones((8, 128), F32)
    for l in range(middle):
        new = diag[l] * old if older is None else diag[l] * old - c[l] * c[l] * older
        inverse[l] = old / new
        older, old = old, new
    older, old = None, jnp.ones((8, 128), F32)
    for l in range(levels - 1, middle, -1):
        new = diag[l] * old if older is None else diag[l] * old - c[l + 1] * c[l + 1] * older
        inverse[l] = old / new
        older, old = old, new
    m = middle
    inverse[m] = 1.0 / (
        diag[m] - c[m] * c[m] * inverse[m - 1] - c[m + 1] * c[m + 1] * inverse[m + 1]
    )
    for l in range(levels):
        inv_ref[8 * l : 8 * l + 8, :] = inverse[l]
        al_ref[8 * l : 8 * l + 8, :] = c[l] * inverse[l]
        be_ref[8 * l : 8 * l + 8, :] = c[l + 1] * inverse[l]

    def substep(n, carry):
        here = n * (levels * 8)
        there = here + levels * 8

        def source(l):
            p = hist_ref[pl.ds(pl.multiple_of(here + 8 * l, 8), 8), :]
            right = a_up(p)
            left = a_dn(p)
            t = row(t_ref, l) + mid_coef * p
            t = t + (out_coef[0] * right + in_coef[0] * left)
            t = t + (out_coef[1] * b_up(p) + in_coef[1] * b_dn(p))
            t = t + (out_coef[2] * b_dn(right) + in_coef[2] * b_up(left))
            t_ref[8 * l : 8 * l + 8, :] = t
            return (p + t) * row(inv_ref, l)

        def put(l, value):
            hist_ref[pl.ds(pl.multiple_of(there + 8 * l, 8), 8), :] = value

        low = high = None
        for l in range(middle):
            h = levels - 1 - l
            low = source(l) if low is None else source(l) + row(al_ref, l) * low
            high = source(h) if high is None else source(h) + row(be_ref, h) * high
            f_ref[8 * l : 8 * l + 8, :] = low
            f_ref[8 * h : 8 * h + 8, :] = high
        low = high = source(middle) + row(al_ref, middle) * low + row(be_ref, middle) * high
        put(middle, low)
        for l in range(middle - 1, -1, -1):
            h = levels - 1 - l
            low = row(f_ref, l) + row(be_ref, l) * low
            high = row(f_ref, h) + row(al_ref, h) * high
            put(l, low)
            put(h, high)
        return carry

    lax.fori_loop(0, SUBSTEPS, substep, 0)

    scale = [g * (1.0 / SUBSTEPS) for g in grad]
    drain = tracer_scale * area

    def finish(l, carry):
        at = pl.ds(pl.multiple_of(8 * l, 8), 8)
        total = None
        weighted = None
        for n in range(SUBSTEPS):
            p = hist_ref[pl.ds(pl.multiple_of(8 * (levels * n + l), 8), 8), :]
            total = p if total is None else total + p
            weighted = total if weighted is None else weighted + total
        out_ref[at, :] = hist_ref[pl.ds(pl.multiple_of(8 * (levels * SUBSTEPS + l), 8), 8), :]
        toward, away = [], []
        shifted = ups(total)
        weight_shift = ups(weighted)
        for k in range(3):
            dq_ref[pl.ds(pl.multiple_of(8 * (GROUP * k + l), 8), 8), :] = shifted[k] - total
            mean = dyn(big_ref, (3 + k) * GROUP + l) - scale[k] * (weight_shift[k] - weighted)
            toward.append(length[k] * jnp.maximum(mean, 0.0))
            away.append(length[k] * jnp.minimum(mean, 0.0))
        for s in range(species):
            tr = dyn(trc_ref, s * GROUP + l)
            beyond = ups(tr)
            flux = [toward[k] * tr + away[k] * beyond[k] for k in range(3)]
            flux_in = back(*flux)
            spread = (flux[0] - flux_in[0]) + (flux[1] - flux_in[1]) + (flux[2] - flux_in[2])
            out_ref[pl.ds(pl.multiple_of(8 * ((s + 1) * GROUP + l), 8), 8), :] = tr - drain * spread
        return carry

    lax.fori_loop(0, levels, finish, 0, unroll=5)

    place = meta_ref[2:3, 0:CELLS]
    spot = ((place >> 4) << 5) + (place & 15) + DEPTH
    cells = jnp.concatenate([out_ref[pl.ds(2 + s, 4 * GROUP, stride=8), :] for s in range(4)], axis=1)
    cells = pick(cells, one_hot(spot, 512))
    newp_ref[...] = cells[0:levels]
    for s in range(species):
        newt_ref[s] = cells[(s + 1) * GROUP : (s + 1) * GROUP + levels]
    spot = meta_ref[0:1, :]
    turned = jnp.zeros((GROUP, edges), F32)
    for k in range(3):
        place = spot - k * CELLS
        lane_of = ((place >> 4) << 5) + (place & 15) + DEPTH
        lane_of = jnp.where((place >= 0) & (place < CELLS), lane_of, -1)
        part = jnp.concatenate(
            [dq_ref[pl.ds(8 * GROUP * k + 2 + s, GROUP, stride=8), :] for s in range(4)], axis=1
        )
        turned = turned + pick(part, one_hot(lane_of, 512))
    sense = meta_ref[1:2, :].astype(F32)
    newv_ref[...] = vel_ref[...] - (grad_scale * sense * invd_ref[...]) * turned[0:levels]


def passed_along(value, axis, steps):
    count = lax.axis_size(axis)
    pairs = [(source, (source + steps) % count) for source in range(count)]
    return lax.ppermute(value, axis, pairs)


INTERPRET = False


def per_device(
    pressure, velocity, tracers, tendency, pattern, coupling, edge_length, inv_distance, inv_area,
    edge_ends, halo_ends, cell_edges, cell_signs, cell_send, edge_send,
):
    levels, edges = velocity.shape
    species = tracers.shape[0]
    stride = lax.axis_size("blk") // 16
    rows = 6 * GROUP + 8
    trows = species * GROUP
    invd_row = inv_distance[None, :]
    shape = jax.ShapeDtypeStruct
    vmem = pl.BlockSpec(memory_space=pltpu.VMEM)
    own, trc, up, down, east, west, meta = pl.pallas_call(
        prepare,
        out_shape=(
            shape((rows, CELLS), F32), shape((trows, CELLS), F32),
            shape((rows, 128), F32), shape((rows, 128), F32), shape((rows, 128), F32), shape((rows, 128), F32),
            shape((8, edges), I32),
        ),
        in_specs=[pl.BlockSpec(memory_space=pltpu.SMEM)] + [vmem] * 10,
        out_specs=(vmem,) * 7,
        scratch_shapes=[pltpu.VMEM((3 * GROUP + 8 + trows, CELLS), F32), pltpu.VMEM((GROUP + 8, edges), F32)],
        interpret=INTERPRET,
        name="prepare",
    )(
        cell_send, pressure, velocity, tracers, tendency, pattern[None, :], coupling, edge_length[None, :],
        invd_row, inv_area[None, :], edge_ends,
    )
    south = passed_along(up, "blk", stride)
    north = passed_along(down, "blk", -stride)
    blank = jnp.zeros((rows, 70), F32)
    cut = DEPTH * DEPTH
    wide = DEPTH * SIDE
    to_east = jnp.concatenate(
        [east[:, :112], south[:, wide - cut : wide], north[:, wide - cut : wide],
         south[:, wide + 15 : wide + 16], north[:, wide + 15 : wide + 16], blank], axis=1,
    )
    to_west = jnp.concatenate(
        [west[:, :112], south[:, :cut], north[:, :cut],
         south[:, wide : wide + 1], north[:, wide : wide + 1], blank], axis=1,
    )
    from_west = passed_along(to_east, "blk", 1)
    from_east = passed_along(to_west, "blk", -1)
    block = pltpu.VMEM((levels * 8, 128), F32)
    return pl.pallas_call(
        advance,
        out_shape=(
            shape((levels, CELLS), F32), shape((levels, edges), F32), shape((species, levels, CELLS), F32),
        ),
        in_specs=[vmem] * 9,
        out_specs=(vmem,) * 3,
        scratch_shapes=[
            pltpu.VMEM((rows * 8, 128), F32), pltpu.VMEM((trows * 8, 128), F32),
            pltpu.VMEM(((SUBSTEPS + 1) * levels * 8, 128), F32),
            block, block, block, block, block,
            pltpu.VMEM((4 * GROUP * 8, 128), F32), pltpu.VMEM((3 * GROUP * 8, 128), F32),
        ],
        interpret=INTERPRET,
        name="advance",
    )(own, trc, south, north, from_west, from_east, meta, velocity, invd_row)


def solution(mesh):
    both = ("member", "blk")
    in_specs = (
        P(None, both), P(None, both), P(None, None, both), P(None, both), P(both),
        P(None, "blk"), P("blk"), P("blk"), P("blk"),
        P(None, "blk"), P(None, "blk"), P(None, "blk"), P(None, "blk"), P(None, "blk"), P(None, "blk"),
    )
    out_specs = (P(None, both), P(None, both), P(None, None, both))
    return jax.shard_map(
        per_device, mesh=mesh, in_specs=in_specs, out_specs=out_specs, check_vma=False
    )
```

```python
import functools

import jax
import jax.numpy as jnp
from jax import lax
from jax.experimental import pallas as pl
from jax.experimental.pallas import tpu as pltpu
from jax.sharding import PartitionSpec as P

SUBSTEPS = 6
grad_scale = 0.25
spread_scale = 0.25
force_scale = 0.5
tracer_scale = 0.05

SIDE = 16
CELLS = SIDE * SIDE
DEPTH = SUBSTEPS
COL = 32
PAD_A = 8
GROUP = 56
F32 = jnp.float32
BF16 = jnp.bfloat16
I32 = jnp.int32


def iota(shape, dim):
    return lax.broadcasted_iota(I32, shape, dim)


def one_hot(row, count):
    return jnp.where(iota((count, row.shape[1]), 0) == row, 1.0, 0.0).astype(BF16)


def halves(x):
    hi = x.astype(BF16)
    return hi, (x - hi.astype(F32)).astype(BF16)


def dot(x, y):
    return lax.dot_general(x, y, (((1,), (0,)), ((), ())), preferred_element_type=F32)


def dot_t(x, y):
    return lax.dot_general(x, y, (((1,), (1,)), ((), ())), preferred_element_type=F32)


def pick(x, table):
    hi, lo = halves(x)
    return dot(hi, table) + dot(lo, table)


def pick_t(x, table):
    hi, lo = halves(x)
    return dot_t(hi, table) + dot_t(lo, table)


def rows8(*rows):
    width = rows[0].shape[1]
    at = iota((8, width), 0)
    out = jnp.zeros((8, width), F32)
    for number, row in enumerate(rows):
        out = jnp.where(at == number, row, out)
    return out


def flat(ref):
    return ref[...].reshape(1, ref.shape[0])


def sixth(j):
    return (j * 43) >> 8


def prepare(*refs):
    sources, rest = refs[:11], refs[11:]
    own_ref, trcl_ref, up_ref, dn_ref, east_ref, west_ref, meta_ref, x_ref, v_ref = rest[:9]
    send_ref, ends_ref, p_ref, vel_ref, trc_ref, tend_ref, pat_ref, coup_ref, len_ref, invd_ref, ia_ref = rest[9:20]
    arrived = rest[20]
    copies = [pltpu.make_async_copy(src, dst, arrived.at[n]) for n, (src, dst) in enumerate(zip(sources, rest[9:20]))]
    for copy in copies:
        copy.start()
    copies[0].wait()
    copies[1].wait()
    levels = p_ref.shape[0]
    edges = vel_ref.shape[1]
    start = ends_ref[0:1, :]
    end = ends_ref[1:2, :]
    start_hot = one_hot(start, CELLS)
    end_hot = one_hot(end, CELLS)
    joined = dot_t(
        jnp.concatenate([start_hot, end_hot], axis=1), jnp.concatenate([end_hot, start_hot], axis=1)
    )
    same = iota((CELLS, CELLS), 0) == iota((CELLS, CELLS), 1)
    step1 = jnp.where(same, 1.0, jnp.minimum(1.0, joined)).astype(BF16)
    step2 = jnp.minimum(1.0, dot(step1, step1)).astype(BF16)
    step4 = jnp.minimum(1.0, dot(step2, step2)).astype(BF16)
    cell = iota((1, CELLS), 1)
    seeds = []
    for side in (1, 0, 3, 2):
        hit = cell == send_ref[side, 0]
        for s in range(1, SIDE):
            hit = hit | (cell == send_ref[side, s])
        seeds.append(jnp.where(hit, 1.0, 0.0))
    reached = rows8(*seeds)
    for step in (step1, step2, step4):
        wider = jnp.minimum(1.0, dot(reached.astype(BF16), step))
        reached = jnp.concatenate([reached, wider], axis=0)
    far = jnp.zeros((8, CELLS), F32)
    for n in range(SIDE // 2):
        far = far + (1.0 - reached[8 * n : 8 * n + 8])
    half = SIDE // 2
    a = jnp.where(far[0:1] < half, far[0:1], SIDE - 1.0 - far[1:2])
    b = jnp.where(far[2:3] < half, far[2:3], SIDE - 1.0 - far[3:4])
    place = (a * SIDE + b).astype(I32)
    corners = rows8(a, b).astype(BF16)
    at_start = dot(corners, start_hot)
    at_end = dot(corners, end_hot)
    a_s, b_s = at_start[0:1], at_start[1:2]
    a_e, b_e = at_end[0:1], at_end[1:2]
    rim_hot = one_hot(end - CELLS, 6 * SIDE)
    met = dot_t(rows8(b_s, jnp.ones_like(b_s)).astype(BF16), rim_hot)
    rim_b = jnp.where(met[1:2] > 1.5, (met[0:1] - 1.0) * 0.5, met[0:1])
    rim_b = dot(rows8(rim_b).astype(BF16), rim_hot)[0:1]
    outside = end >= CELLS
    peer = (end - CELLS) >> 4
    zero = jnp.zeros_like(end)
    direction_out = jnp.where(
        peer == 3, zero + 1, jnp.where(peer == 1, jnp.where(jnp.abs(b_s - rim_b) < 0.5, zero, zero + 2), zero + 2)
    )
    da = a_e - a_s
    db = b_e - b_s
    direction_in = jnp.where(jnp.abs(db) < 0.5, zero, jnp.where(jnp.abs(da) < 0.5, zero + 1, zero + 2))
    onward = outside | (da > 0.5) | ((jnp.abs(da) < 0.5) & (db > 0.5))
    direction = jnp.where(outside, direction_out, direction_in)
    sense = jnp.where(onward, 1.0, -1.0)
    anchor = jnp.where(onward, a_s * SIDE + b_s, a_e * SIDE + b_e).astype(I32)
    spot = direction * CELLS + anchor
    at8 = iota((8, edges), 0)
    meta = jnp.where(at8 == 0, spot, jnp.where(at8 == 1, sense.astype(I32), zero))
    meta_ref[...] = meta
    meta_ref[2:3, 0:CELLS] = place
    for copy in copies[2:]:
        copy.wait()
    x_ref[...] = jnp.zeros(x_ref.shape, F32)
    height = iota((levels, 1), 0).astype(F32)
    taper = jnp.minimum(1.0, (levels - 1.0 - height) / (0.25 * levels))
    x_ref[0:levels] = p_ref[...]
    x_ref[GROUP : GROUP + levels] = force_scale * (1.0 + flat(pat_ref) * taper) * tend_ref[...]
    x_ref[2 * GROUP : 2 * GROUP + levels] = coup_ref[...]
    x_ref[3 * GROUP : 3 * GROUP + 1] = flat(ia_ref)
    first = 3 * GROUP + 8
    for n in range(trc_ref.shape[0]):
        x_ref[first + n * GROUP : first + n * GROUP + levels] = trc_ref[n]
    place_hot = one_hot(place, CELLS)
    moved = pick_t(x_ref[...], place_hot)
    own_ref[0 : 3 * GROUP] = moved[0 : 3 * GROUP]
    trcl_ref[...] = moved[first:]
    v_ref[...] = jnp.zeros(v_ref.shape, F32)
    v_ref[0:levels] = vel_ref[...] * sense
    v_ref[GROUP : GROUP + 1] = flat(len_ref)
    v_ref[GROUP + 1 : GROUP + 2] = flat(invd_ref)
    v_hi, v_lo = halves(v_ref[...])
    lengths, distances = [], []
    for k in range(3):
        spot_hot = one_hot(spot - k * CELLS, CELLS)
        got = dot_t(v_hi, spot_hot) + dot_t(v_lo, spot_hot)
        own_ref[(3 + k) * GROUP : (4 + k) * GROUP] = got[0:GROUP]
        lengths.append(got[GROUP : GROUP + 1])
        distances.append(got[GROUP + 1 : GROUP + 2])
    own_ref[6 * GROUP : 6 * GROUP + 8] = rows8(*lengths, *distances, moved[3 * GROUP : 3 * GROUP + 1])
    column = iota((1, 512), 1)
    part = column >> 7
    j = column & 127
    sa = sixth(j)
    sb = j - sa * 6
    strip = jnp.where(
        part == 0, sa * SIDE + SIDE - DEPTH + sb,
        jnp.where(part == 1, sa * SIDE + sb, jnp.where(part == 2, j + CELLS - DEPTH * SIDE, j)),
    )
    strip = jnp.where(j < DEPTH * SIDE, strip, -1)
    t = j - DEPTH * SIDE
    rim = jnp.where(
        part == 0, t * SIDE + SIDE - 1, jnp.where(part == 1, t * SIDE, jnp.where(part == 2, t + CELLS - SIDE, t))
    )
    rim = jnp.where((t >= 0) & (t < SIDE), rim, -1)
    strips = pick(own_ref[...], one_hot(strip, CELLS))
    rims = pick(trcl_ref[...], one_hot(rim, CELLS))
    top = strips[0 : rims.shape[0]] + rims
    rest = strips[rims.shape[0] :]
    for number, ref in enumerate((up_ref, dn_ref, east_ref, west_ref)):
        ref[0 : rims.shape[0]] = top[:, 128 * number : 128 * number + 128]
        ref[rims.shape[0] :] = rest[:, 128 * number : 128 * number + 128]


def pack(east_ref, west_ref, south_ref, north_ref, to_east_ref, to_west_ref):
    rows = east_ref.shape[0]
    split = rows - to_east_ref.shape[0]
    cut = DEPTH * DEPTH
    wide = DEPTH * SIDE
    rim = wide + SIDE
    for part, out, body, corner in (
        (east_ref, to_east_ref, wide - cut, rim - 1), (west_ref, to_west_ref, 0, wide),
    ):
        out[split:, 0:256] = jnp.zeros((out.shape[0] - split, 256), F32)
        for begin, end, at in ((0, split, 0), (split, rows, 192)):
            count = end - begin
            line = [
                part[begin:end, 0:rim], south_ref[begin:end, body : body + cut],
                north_ref[begin:end, body : body + cut], south_ref[begin:end, corner : corner + 1],
                north_ref[begin:end, corner : corner + 1], jnp.zeros((count, 6), F32),
            ]
            out[0:count, at : at + 192] = jnp.concatenate(line, axis=1)


def advance(
    own_ref, trcl_ref, south_ref, north_ref, west_ref, east_ref, meta_ref, vel_ref, invd_ref,
    newp_ref, newv_ref, newt_ref,
    big_ref, trc_ref, hist_ref, t_ref, f_ref, inv_ref, al_ref, be_ref, out_ref, dq_ref, flow_ref,
):
    levels = newp_ref.shape[0]
    species = newt_ref.shape[0]
    edges = newv_ref.shape[1]
    rows = own_ref.shape[0]
    trows = trcl_ref.shape[0]
    q = iota((1, 512), 1)
    qa = q >> 5
    qb = (q & 31) - DEPTH
    inside = (qb >= 0) & (qb < SIDE)
    below = (qb >= -DEPTH) & (qb < 0)
    above = (qb >= SIDE) & (qb < SIDE + DEPTH)
    src = jnp.where(inside, qa * SIDE + qb, -1)
    rsrc = jnp.where(below, qa * DEPTH + qb + DEPTH, jnp.where(above, 128 + qa * DEPTH + qb - SIDE, -1))
    tsrc = jnp.where(qb == -1, 96 + qa, jnp.where(qb == SIDE, 128 + 96 + qa, -1))
    sn_hi, sn_lo = halves(jnp.concatenate([south_ref[...], north_ref[...]], axis=1))
    own_hot = one_hot(src, 256)
    rim_hot = one_hot(rsrc, 256)
    core = pick(own_ref[...], own_hot) + (dot(sn_hi, rim_hot) + dot(sn_lo, rim_hot))
    rim_hot = one_hot(tsrc, 256)
    tcore = pick(trcl_ref[...], own_hot) + (dot(sn_hi[0:trows], rim_hot) + dot(sn_lo[0:trows], rim_hot))
    for s in range(4):
        big_ref[pl.ds(2 + s, rows, stride=8), :] = core[:, 128 * s : 128 * s + 128]
        trc_ref[pl.ds(2 + s, trows, stride=8), :] = tcore[:, 128 * s : 128 * s + 128]
    q = iota((1, 256), 1)
    qb = (q & 31) - DEPTH
    inside = (qb >= 0) & (qb < SIDE)
    below = (qb >= -DEPTH) & (qb < 0)
    above = (qb >= SIDE) & (qb < SIDE + DEPTH)
    for side, ref in ((0, west_ref), (6, east_ref)):
        qa = (q >> 5) - (PAD_A - DEPTH if side == 0 else 0)
        src = jnp.where(
            inside, qa * SIDE + qb,
            jnp.where(below, 112 + qa * DEPTH + qb + DEPTH, jnp.where(above, 148 + qa * DEPTH + qb - SIDE, -1)),
        )
        src = jnp.where((qa >= 0) & (qa < DEPTH), src, -1)
        near = DEPTH - 1 if side == 0 else 0
        tsrc = jnp.where(
            inside, 96 + qb, jnp.where(qb == -1, 184, jnp.where(qb == SIDE, 185, -1))
        )
        tsrc = jnp.where(qa == near, tsrc, -1)
        hi, lo = halves(ref[...])
        hot = one_hot(src, 256)
        thot = one_hot(tsrc, 256)
        late_hot = one_hot(jnp.where(src >= 0, src + 64, -1), 256)
        flank = dot(hi[0:trows, 0:256], hot) + dot(lo[0:trows, 0:256], hot)
        late = dot(hi[:, 128:384], late_hot) + dot(lo[:, 128:384], late_hot)
        tflank = dot(hi[0:trows, 0:256], thot) + dot(lo[0:trows, 0:256], thot)
        for s in range(2):
            cut = slice(128 * s, 128 * s + 128)
            big_ref[pl.ds(side + s, trows, stride=8), :] = flank[:, cut]
            big_ref[pl.ds(8 * trows + side + s, rows - trows, stride=8), :] = late[:, cut]
            trc_ref[pl.ds(side + s, trows, stride=8), :] = tflank[:, cut]

    lane = iota((8, 128), 1)

    def ahead(x, step):
        y = pltpu.roll(x, 128 - step, 1)
        return jnp.where(lane >= 128 - step, pltpu.roll(y, 7, 0), y)

    def behind(x, step):
        y = pltpu.roll(x, step, 1)
        return jnp.where(lane < step, pltpu.roll(y, 1, 0), y)

    def ups(x):
        return ahead(x, COL), pltpu.roll(x, 127, 1), ahead(x, COL - 1)

    def back(x0, x1, x2):
        return behind(x0, COL), pltpu.roll(x1, 1, 1), behind(x2, COL - 1)

    def row(ref, number):
        return ref[8 * number : 8 * number + 8, :]

    def dyn(ref, number):
        return ref[pl.ds(pl.multiple_of(8 * number, 8), 8), :]

    length = [row(big_ref, 6 * GROUP + k) for k in range(3)]
    grad = [grad_scale * row(big_ref, 6 * GROUP + 3 + k) for k in range(3)]
    area = row(big_ref, 6 * GROUP + 6)
    pull = spread_scale * area
    out_coef = [length[k] * grad[k] for k in range(3)]
    in_coef = back(*out_coef)
    out_coef = [pull * c for c in out_coef]
    in_coef = [pull * c for c in in_coef]
    mid_coef = -(out_coef[0] + out_coef[1] + out_coef[2] + in_coef[0] + in_coef[1] + in_coef[2])

    def first_spread(l, carry):
        w = [length[k] * dyn(big_ref, (3 + k) * GROUP + l) for k in range(3)]
        w_in = back(*w)
        total = (w[0] - w_in[0]) + (w[1] - w_in[1]) + (w[2] - w_in[2])
        at = pl.ds(pl.multiple_of(8 * l, 8), 8)
        t_ref[at, :] = dyn(big_ref, GROUP + l) - pull * total
        hist_ref[at, :] = dyn(big_ref, l)
        return carry

    lax.fori_loop(0, levels, first_spread, 0, unroll=55)

    middle = levels // 2
    c = [row(big_ref, 2 * GROUP + l) for l in range(levels)] + [jnp.zeros((8, 128), F32)]
    diag = [1.0 + c[l] + c[l + 1] for l in range(levels)]
    inverse = [None] * levels
    older, old = None, jnp.ones((8, 128), F32)
    for l in range(middle):
        new = diag[l] * old if older is None else diag[l] * old - c[l] * c[l] * older
        inverse[l] = old / new
        older, old = old, new
    older, old = None, jnp.ones((8, 128), F32)
    for l in range(levels - 1, middle, -1):
        new = diag[l] * old if older is None else diag[l] * old - c[l + 1] * c[l + 1] * older
        inverse[l] = old / new
        older, old = old, new
    m = middle
    inverse[m] = 1.0 / (
        diag[m] - c[m] * c[m] * inverse[m - 1] - c[m + 1] * c[m + 1] * inverse[m + 1]
    )
    for l in range(levels):
        inv_ref[8 * l : 8 * l + 8, :] = inverse[l]
        al_ref[8 * l : 8 * l + 8, :] = c[l] * inverse[l]
        be_ref[8 * l : 8 * l + 8, :] = c[l + 1] * inverse[l]

    def substep(n, carry):
        here = n * (levels * 8)
        there = here + levels * 8

        def source(l):
            p = hist_ref[pl.ds(pl.multiple_of(here + 8 * l, 8), 8), :]
            fore = ups(p)
            rear = back(p, p, p)
            t = row(t_ref, l) + mid_coef * p
            for k in range(3):
                t = t + (out_coef[k] * fore[k] + in_coef[k] * rear[k])
            t_ref[8 * l : 8 * l + 8, :] = t
            f_ref[8 * l : 8 * l + 8, :] = (p + t) * row(inv_ref, l)

        def put(l, value):
            hist_ref[pl.ds(pl.multiple_of(there + 8 * l, 8), 8), :] = value

        for l in range(levels):
            source(l)
        low, high = row(f_ref, 0), row(f_ref, levels - 1)
        for l in range(1, middle):
            h = levels - 1 - l
            low = row(f_ref, l) + row(al_ref, l) * low
            high = row(f_ref, h) + row(be_ref, h) * high
            f_ref[8 * l : 8 * l + 8, :] = low
            f_ref[8 * h : 8 * h + 8, :] = high
        low = high = row(f_ref, middle) + row(al_ref, middle) * low + row(be_ref, middle) * high
        put(middle, low)
        for l in range(middle - 1, -1, -1):
            h = levels - 1 - l
            low = row(f_ref, l) + row(be_ref, l) * low
            high = row(f_ref, h) + row(al_ref, h) * high
            put(l, low)
            put(h, high)
        return carry

    lax.fori_loop(0, SUBSTEPS, substep, 0)

    scale = [g * (1.0 / SUBSTEPS) for g in grad]
    drain = tracer_scale * area

    def finish(l, carry):
        at = pl.ds(pl.multiple_of(8 * l, 8), 8)
        total = None
        weighted = None
        for n in range(SUBSTEPS):
            p = hist_ref[pl.ds(pl.multiple_of(8 * (levels * n + l), 8), 8), :]
            total = p if total is None else total + p
            weighted = total if weighted is None else weighted + total
        out_ref[at, :] = hist_ref[pl.ds(pl.multiple_of(8 * (levels * SUBSTEPS + l), 8), 8), :]
        shifted = ups(total)
        weight_shift = ups(weighted)
        for k in range(3):
            dq_ref[pl.ds(pl.multiple_of(8 * (GROUP * k + l), 8), 8), :] = shifted[k] - total
            mean = dyn(big_ref, (3 + k) * GROUP + l) - scale[k] * (weight_shift[k] - weighted)
            flow_ref[pl.ds(pl.multiple_of(8 * (GROUP * k + l), 8), 8), :] = length[k] * jnp.maximum(mean, 0.0)
            flow_ref[pl.ds(pl.multiple_of(8 * (GROUP * (3 + k) + l), 8), 8), :] = length[k] * jnp.minimum(mean, 0.0)
        return carry

    lax.fori_loop(0, levels, finish, 0, unroll=55)

    def carry_tracers(l, carry):
        toward = [dyn(flow_ref, GROUP * k + l) for k in range(3)]
        away = [dyn(flow_ref, GROUP * (3 + k) + l) for k in range(3)]
        toward_in = back(*toward)
        away_in = back(*away)
        keep = (toward[0] - away_in[0]) + (toward[1] - away_in[1]) + (toward[2] - away_in[2])
        for s in range(species):
            tr = dyn(trc_ref, s * GROUP + l)
            beyond = ups(tr)
            before = back(tr, tr, tr)
            spread = keep * tr
            for k in range(3):
                spread = spread + (away[k] * beyond[k] - toward_in[k] * before[k])
            out_ref[pl.ds(pl.multiple_of(8 * ((s + 1) * GROUP + l), 8), 8), :] = tr - drain * spread
        return carry

    lax.fori_loop(0, levels, carry_tracers, 0, unroll=55)

    kept = (iota((1, 128), 1) & 31) - DEPTH
    kept = (kept >= 0) & (kept < SIDE)

    def folded(ref, begin, count):
        blocks = [ref[pl.ds(8 * begin + 2 + s, count, stride=8), :] for s in range(4)]
        pairs = [jnp.where(kept, blocks[s], pltpu.roll(blocks[s + 1], SIDE, 1)) for s in (0, 2)]
        return jnp.concatenate(pairs, axis=1)

    def lane_of(place):
        column = place >> 4
        at = ((column & 3) << 5) + (place & 15) + DEPTH + ((column >> 2) & 1) * SIDE
        return ((column >> 3) << 7) + (at & 127)

    cells = pick(folded(out_ref, 0, 4 * GROUP), one_hot(lane_of(meta_ref[2:3, 0:CELLS]), 256))
    newp_ref[...] = cells[0:levels]
    for s in range(species):
        newt_ref[s] = cells[(s + 1) * GROUP : (s + 1) * GROUP + levels]
    spot = meta_ref[0:1, :]
    turned = jnp.zeros((GROUP, edges), F32)
    for k in range(3):
        place = spot - k * CELLS
        at = jnp.where((place >= 0) & (place < CELLS), lane_of(place & (CELLS - 1)), -1)
        turned = turned + pick(folded(dq_ref, GROUP * k, GROUP), one_hot(at, 256))
    sense = meta_ref[1:2, :].astype(F32)
    newv_ref[...] = vel_ref[...] - (grad_scale * sense * flat(invd_ref)) * turned[0:levels]


def passed_along(value, axis, steps):
    count = lax.axis_size(axis)
    pairs = [(source, (source + steps) % count) for source in range(count)]
    return lax.ppermute(value, axis, pairs)


INTERPRET = False


def per_device(
    pressure, velocity, tracers, tendency, pattern, coupling, edge_length, inv_distance, inv_area,
    edge_ends, halo_ends, cell_edges, cell_signs, cell_send, edge_send,
):
    levels, edges = velocity.shape
    species = tracers.shape[0]
    stride = lax.axis_size("blk") // 16
    rows = 6 * GROUP + 8
    trows = species * GROUP
    shape = jax.ShapeDtypeStruct
    vmem = pl.BlockSpec(memory_space=pltpu.VMEM)
    inputs = (
        cell_send, edge_ends, pressure, velocity, tracers, tendency, pattern, coupling, edge_length,
        inv_distance, inv_area,
    )
    inputs = [pltpu.with_memory_space_constraint(array, pltpu.HBM) for array in inputs]
    own, trc, up, down, east, west, meta = pl.pallas_call(
        prepare,
        out_shape=(
            shape((rows, CELLS), F32), shape((trows, CELLS), F32),
            shape((rows, 128), F32), shape((rows, 128), F32), shape((rows, 128), F32), shape((rows, 128), F32),
            shape((8, edges), I32),
        ),
        in_specs=[pl.BlockSpec(memory_space=pltpu.HBM)] * 11,
        out_specs=(vmem,) * 7,
        scratch_shapes=[
            pltpu.VMEM((3 * GROUP + 8 + trows, CELLS), F32), pltpu.VMEM((GROUP + 8, edges), F32),
            pltpu.SMEM(cell_send.shape, I32),
        ] + [pltpu.VMEM(array.shape, array.dtype) for array in inputs[1:]] + [pltpu.SemaphoreType.DMA((11,))],
        compiler_params=pltpu.CompilerParams(vmem_limit_bytes=40 * 2**20),
        interpret=INTERPRET,
        name="prepare",
    )(*inputs)
    south = passed_along(up, "blk", stride)
    north = passed_along(down, "blk", -stride)
    half = shape((rows - trows, 384), F32)
    to_east, to_west = pl.pallas_call(
        pack,
        out_shape=(half, half),
        in_specs=[vmem] * 4,
        out_specs=(vmem,) * 2,
        compiler_params=pltpu.CompilerParams(vmem_limit_bytes=40 * 2**20),
        interpret=INTERPRET,
        name="pack",
    )(east, west, south, north)
    from_west = passed_along(to_east, "blk", 1)
    from_east = passed_along(to_west, "blk", -1)
    block = pltpu.VMEM((levels * 8, 128), F32)
    return pl.pallas_call(
        advance,
        out_shape=(
            shape((levels, CELLS), F32), shape((levels, edges), F32), shape((species, levels, CELLS), F32),
        ),
        in_specs=[vmem] * 9,
        out_specs=(vmem,) * 3,
        scratch_shapes=[
            pltpu.VMEM((rows * 8, 128), F32), pltpu.VMEM((trows * 8, 128), F32),
            pltpu.VMEM(((SUBSTEPS + 1) * levels * 8, 128), F32),
            block, block, block, block, block,
            pltpu.VMEM((4 * GROUP * 8, 128), F32), pltpu.VMEM((3 * GROUP * 8, 128), F32),
            pltpu.VMEM((6 * GROUP * 8, 128), F32),
        ],
        compiler_params=pltpu.CompilerParams(vmem_limit_bytes=40 * 2**20),
        interpret=INTERPRET,
        name="advance",
    )(own, trc, south, north, from_west, from_east, meta, velocity, inv_distance)


def solution(mesh):
    both = ("member", "blk")
    in_specs = (
        P(None, both), P(None, both), P(None, None, both), P(None, both), P(both),
        P(None, "blk"), P("blk"), P("blk"), P("blk"),
        P(None, "blk"), P(None, "blk"), P(None, "blk"), P(None, "blk"), P(None, "blk"), P(None, "blk"),
    )
    out_specs = (P(None, both), P(None, both), P(None, None, both))
    return jax.shard_map(
        per_device, mesh=mesh, in_specs=in_specs, out_specs=out_specs, check_vma=False
    )
```

```python
import jax
import jax.numpy as jnp
from jax import lax
from jax.experimental import pallas as pl
from jax.experimental.pallas import tpu as pltpu
from jax.sharding import PartitionSpec as P


SUBSTEPS = 6
grad_scale = 0.25
spread_scale = 0.25
force_scale = 0.5
tracer_scale = 0.05

SIDE = 16
CELLS = SIDE * SIDE
DEPTH = SUBSTEPS
COL = 32
PAD_A = 8
GROUP = 56
F32 = jnp.float32
BF16 = jnp.bfloat16
I32 = jnp.int32


def iota(shape, dim):
    return lax.broadcasted_iota(I32, shape, dim)


def one_hot(row, count):
    return jnp.where(iota((count, row.shape[1]), 0) == row, 1.0, 0.0).astype(BF16)


def halves(x):
    hi = x.astype(BF16)
    return hi, (x - hi.astype(F32)).astype(BF16)


def dot(x, y):
    return lax.dot_general(x, y, (((1,), (0,)), ((), ())), preferred_element_type=F32)


def dot_t(x, y):
    return lax.dot_general(x, y, (((1,), (1,)), ((), ())), preferred_element_type=F32)


def pick(x, table):
    hi, lo = halves(x)
    return dot(hi, table) + dot(lo, table)


def pick_t(x, table):
    hi, lo = halves(x)
    return dot_t(hi, table) + dot_t(lo, table)


def rows8(*rows):
    width = rows[0].shape[1]
    at = iota((8, width), 0)
    out = jnp.zeros((8, width), F32)
    for number, row in enumerate(rows):
        out = jnp.where(at == number, row, out)
    return out


def flat(ref):
    return ref[...].reshape(1, ref.shape[0])


def sixth(j):
    return (j * 43) >> 8


def prepare(*refs):
    sources, rest = refs[:11], refs[11:]
    own_ref, trcl_ref, up_ref, dn_ref, east_ref, west_ref, meta_ref, x_ref, v_ref = rest[:9]
    send_ref, ends_ref, p_ref, vel_ref, trc_ref, tend_ref, pat_ref, coup_ref, len_ref, invd_ref, ia_ref = rest[9:20]
    arrived = rest[20]
    copies = [pltpu.make_async_copy(src, dst, arrived.at[n]) for n, (src, dst) in enumerate(zip(sources, rest[9:20]))]
    for copy in copies:
        copy.start()
    copies[0].wait()
    copies[1].wait()
    levels = p_ref.shape[0]
    edges = vel_ref.shape[1]
    start = ends_ref[0:1, :]
    end = ends_ref[1:2, :]
    start_hot = one_hot(start, CELLS)
    end_hot = one_hot(end, CELLS)
    joined = dot_t(
        jnp.concatenate([start_hot, end_hot], axis=1), jnp.concatenate([end_hot, start_hot], axis=1)
    )
    same = iota((CELLS, CELLS), 0) == iota((CELLS, CELLS), 1)
    step1 = jnp.where(same, 1.0, jnp.minimum(1.0, joined)).astype(BF16)
    step2 = jnp.minimum(1.0, dot(step1, step1)).astype(BF16)
    step4 = jnp.minimum(1.0, dot(step2, step2)).astype(BF16)
    cell = iota((1, CELLS), 1)
    seeds = []
    for side in (1, 0, 3, 2):
        hit = cell == send_ref[side, 0]
        for s in range(1, SIDE):
            hit = hit | (cell == send_ref[side, s])
        seeds.append(jnp.where(hit, 1.0, 0.0))
    reached = rows8(*seeds)
    for step in (step1, step2, step4):
        wider = jnp.minimum(1.0, dot(reached.astype(BF16), step))
        reached = jnp.concatenate([reached, wider], axis=0)
    far = jnp.zeros((8, CELLS), F32)
    for n in range(SIDE // 2):
        far = far + (1.0 - reached[8 * n : 8 * n + 8])
    half = SIDE // 2
    a = jnp.where(far[0:1] < half, far[0:1], SIDE - 1.0 - far[1:2])
    b = jnp.where(far[2:3] < half, far[2:3], SIDE - 1.0 - far[3:4])
    place = (a * SIDE + b).astype(I32)
    corners = rows8(a, b).astype(BF16)
    at_start = dot(corners, start_hot)
    at_end = dot(corners, end_hot)
    a_s, b_s = at_start[0:1], at_start[1:2]
    a_e, b_e = at_end[0:1], at_end[1:2]
    rim_hot = one_hot(end - CELLS, 6 * SIDE)
    met = dot_t(rows8(b_s, jnp.ones_like(b_s)).astype(BF16), rim_hot)
    rim_b = jnp.where(met[1:2] > 1.5, (met[0:1] - 1.0) * 0.5, met[0:1])
    rim_b = dot(rows8(rim_b).astype(BF16), rim_hot)[0:1]
    outside = end >= CELLS
    peer = (end - CELLS) >> 4
    zero = jnp.zeros_like(end)
    direction_out = jnp.where(
        peer == 3, zero + 1, jnp.where(peer == 1, jnp.where(jnp.abs(b_s - rim_b) < 0.5, zero, zero + 2), zero + 2)
    )
    da = a_e - a_s
    db = b_e - b_s
    direction_in = jnp.where(jnp.abs(db) < 0.5, zero, jnp.where(jnp.abs(da) < 0.5, zero + 1, zero + 2))
    onward = outside | (da > 0.5) | ((jnp.abs(da) < 0.5) & (db > 0.5))
    direction = jnp.where(outside, direction_out, direction_in)
    sense = jnp.where(onward, 1.0, -1.0)
    anchor = jnp.where(onward, a_s * SIDE + b_s, a_e * SIDE + b_e).astype(I32)
    spot = direction * CELLS + anchor
    at8 = iota((8, edges), 0)
    meta = jnp.where(at8 == 0, spot, jnp.where(at8 == 1, sense.astype(I32), zero))
    meta_ref[...] = meta
    meta_ref[2:3, 0:CELLS] = place
    for copy in copies[2:]:
        copy.wait()
    x_ref[...] = jnp.zeros(x_ref.shape, F32)
    height = iota((levels, 1), 0).astype(F32)
    taper = jnp.minimum(1.0, (levels - 1.0 - height) / (0.25 * levels))
    x_ref[0:levels] = p_ref[...]
    x_ref[GROUP : GROUP + levels] = force_scale * (1.0 + flat(pat_ref) * taper) * tend_ref[...]
    x_ref[2 * GROUP : 2 * GROUP + levels] = coup_ref[...]
    x_ref[3 * GROUP : 3 * GROUP + 1] = flat(ia_ref)
    first = 3 * GROUP + 8
    for n in range(trc_ref.shape[0]):
        x_ref[first + n * GROUP : first + n * GROUP + levels] = trc_ref[n]
    place_hot = one_hot(place, CELLS)
    moved = pick_t(x_ref[...], place_hot)
    own_ref[0 : 3 * GROUP] = moved[0 : 3 * GROUP]
    trcl_ref[...] = moved[first:]
    v_ref[...] = jnp.zeros(v_ref.shape, F32)
    v_ref[0:levels] = vel_ref[...] * sense
    v_ref[GROUP : GROUP + 1] = flat(len_ref)
    v_ref[GROUP + 1 : GROUP + 2] = flat(invd_ref)
    v_hi, v_lo = halves(v_ref[...])
    lengths, distances = [], []
    for k in range(3):
        spot_hot = one_hot(spot - k * CELLS, CELLS)
        got = dot_t(v_hi, spot_hot) + dot_t(v_lo, spot_hot)
        own_ref[(3 + k) * GROUP : (4 + k) * GROUP] = got[0:GROUP]
        lengths.append(got[GROUP : GROUP + 1])
        distances.append(got[GROUP + 1 : GROUP + 2])
    own_ref[6 * GROUP : 6 * GROUP + 8] = rows8(*lengths, *distances, moved[3 * GROUP : 3 * GROUP + 1])
    column = iota((1, 512), 1)
    part = column >> 7
    j = column & 127
    sa = sixth(j)
    sb = j - sa * 6
    strip = jnp.where(
        part == 0, sa * SIDE + SIDE - DEPTH + sb,
        jnp.where(part == 1, sa * SIDE + sb, jnp.where(part == 2, j + CELLS - DEPTH * SIDE, j)),
    )
    strip = jnp.where(j < DEPTH * SIDE, strip, -1)
    t = j - DEPTH * SIDE
    rim = jnp.where(
        part == 0, t * SIDE + SIDE - 1, jnp.where(part == 1, t * SIDE, jnp.where(part == 2, t + CELLS - SIDE, t))
    )
    rim = jnp.where((t >= 0) & (t < SIDE), rim, -1)
    strips = pick(own_ref[...], one_hot(strip, CELLS))
    rims = pick(trcl_ref[...], one_hot(rim, CELLS))
    top = strips[0 : rims.shape[0]] + rims
    rest = strips[rims.shape[0] :]
    for number, ref in enumerate((up_ref, dn_ref, east_ref, west_ref)):
        ref[0 : rims.shape[0]] = top[:, 128 * number : 128 * number + 128]
        ref[rims.shape[0] :] = rest[:, 128 * number : 128 * number + 128]


def pack(east_ref, west_ref, south_ref, north_ref, to_east_ref, to_west_ref):
    rows = east_ref.shape[0]
    split = rows - to_east_ref.shape[0]
    cut = DEPTH * DEPTH
    wide = DEPTH * SIDE
    rim = wide + SIDE
    for part, out, body, corner in (
        (east_ref, to_east_ref, wide - cut, rim - 1), (west_ref, to_west_ref, 0, wide),
    ):
        out[split:, 0:256] = jnp.zeros((out.shape[0] - split, 256), F32)
        for begin, end, at in ((0, split, 0), (split, rows, 192)):
            count = end - begin
            line = [
                part[begin:end, 0:rim], south_ref[begin:end, body : body + cut],
                north_ref[begin:end, body : body + cut], south_ref[begin:end, corner : corner + 1],
                north_ref[begin:end, corner : corner + 1], jnp.zeros((count, 6), F32),
            ]
            out[0:count, at : at + 192] = jnp.concatenate(line, axis=1)


def settle(own_ref, trcl_ref, south_ref, north_ref, meta_ref, core_ref, tcore_ref, cell_hot_ref, edge_hot_ref):
    trows = trcl_ref.shape[0]
    q = iota((1, 512), 1)
    qa = q >> 5
    qb = (q & 31) - DEPTH
    inside = (qb >= 0) & (qb < SIDE)
    below = (qb >= -DEPTH) & (qb < 0)
    above = (qb >= SIDE) & (qb < SIDE + DEPTH)
    src = jnp.where(inside, qa * SIDE + qb, -1)
    rsrc = jnp.where(below, qa * DEPTH + qb + DEPTH, jnp.where(above, 128 + qa * DEPTH + qb - SIDE, -1))
    tsrc = jnp.where(qb == -1, 96 + qa, jnp.where(qb == SIDE, 128 + 96 + qa, -1))
    sn_hi, sn_lo = halves(jnp.concatenate([south_ref[...], north_ref[...]], axis=1))
    own_hot = one_hot(src, 256)
    rim_hot = one_hot(rsrc, 256)
    core_ref[...] = pick(own_ref[...], own_hot) + (dot(sn_hi, rim_hot) + dot(sn_lo, rim_hot))
    rim_hot = one_hot(tsrc, 256)
    tcore_ref[...] = pick(trcl_ref[...], own_hot) + (dot(sn_hi[0:trows], rim_hot) + dot(sn_lo[0:trows], rim_hot))

    def lane_of(place):
        column = place >> 4
        at = ((column & 3) << 5) + (place & 15) + DEPTH + ((column >> 2) & 1) * SIDE
        return ((column >> 3) << 7) + (at & 127)

    cell_hot_ref[...] = one_hot(lane_of(meta_ref[2:3, 0:CELLS]), 256)
    spot = meta_ref[0:1, :]
    for k in range(3):
        place = spot - k * CELLS
        at = jnp.where((place >= 0) & (place < CELLS), lane_of(place & (CELLS - 1)), -1)
        edge_hot_ref[256 * k : 256 * k + 256] = one_hot(at, 256)


def advance(
    core_ref, tcore_ref, west_ref, east_ref, cell_hot_ref, edge_hot_ref, meta_ref, vel_ref, invd_ref,
    newp_ref, newv_ref, newt_ref,
    big_ref, trc_ref, hist_ref, t_ref, f_ref, inv_ref, al_ref, be_ref, out_ref, dq_ref, flow_ref,
):
    levels = newp_ref.shape[0]
    species = newt_ref.shape[0]
    edges = newv_ref.shape[1]
    rows = core_ref.shape[0]
    trows = tcore_ref.shape[0]
    for s in range(4):
        big_ref[pl.ds(2 + s, rows, stride=8), :] = core_ref[:, 128 * s : 128 * s + 128]
        trc_ref[pl.ds(2 + s, trows, stride=8), :] = tcore_ref[:, 128 * s : 128 * s + 128]
    q = iota((1, 256), 1)
    qb = (q & 31) - DEPTH
    inside = (qb >= 0) & (qb < SIDE)
    below = (qb >= -DEPTH) & (qb < 0)
    above = (qb >= SIDE) & (qb < SIDE + DEPTH)
    for side, ref in ((0, west_ref), (6, east_ref)):
        qa = (q >> 5) - (PAD_A - DEPTH if side == 0 else 0)
        src = jnp.where(
            inside, qa * SIDE + qb,
            jnp.where(below, 112 + qa * DEPTH + qb + DEPTH, jnp.where(above, 148 + qa * DEPTH + qb - SIDE, -1)),
        )
        src = jnp.where((qa >= 0) & (qa < DEPTH), src, -1)
        near = DEPTH - 1 if side == 0 else 0
        tsrc = jnp.where(
            inside, 96 + qb, jnp.where(qb == -1, 184, jnp.where(qb == SIDE, 185, -1))
        )
        tsrc = jnp.where(qa == near, tsrc, -1)
        hi, lo = halves(ref[...])
        hot = one_hot(src, 256)
        thot = one_hot(tsrc, 256)
        late_hot = one_hot(jnp.where(src >= 0, src + 64, -1), 256)
        flank = dot(hi[0:trows, 0:256], hot) + dot(lo[0:trows, 0:256], hot)
        late = dot(hi[:, 128:384], late_hot) + dot(lo[:, 128:384], late_hot)
        tflank = dot(hi[0:trows, 0:256], thot) + dot(lo[0:trows, 0:256], thot)
        for s in range(2):
            cut = slice(128 * s, 128 * s + 128)
            big_ref[pl.ds(side + s, trows, stride=8), :] = flank[:, cut]
            big_ref[pl.ds(8 * trows + side + s, rows - trows, stride=8), :] = late[:, cut]
            trc_ref[pl.ds(side + s, trows, stride=8), :] = tflank[:, cut]

    lane = iota((8, 128), 1)

    def ahead(x, step):
        y = pltpu.roll(x, 128 - step, 1)
        return jnp.where(lane >= 128 - step, pltpu.roll(y, 7, 0), y)

    def behind(x, step):
        y = pltpu.roll(x, step, 1)
        return jnp.where(lane < step, pltpu.roll(y, 1, 0), y)

    def ups(x):
        return ahead(x, COL), pltpu.roll(x, 127, 1), ahead(x, COL - 1)

    def back(x0, x1, x2):
        return behind(x0, COL), pltpu.roll(x1, 1, 1), behind(x2, COL - 1)

    def row(ref, number):
        return ref[8 * number : 8 * number + 8, :]

    def dyn(ref, number):
        return ref[pl.ds(pl.multiple_of(8 * number, 8), 8), :]

    length = [row(big_ref, 6 * GROUP + k) for k in range(3)]
    grad = [grad_scale * row(big_ref, 6 * GROUP + 3 + k) for k in range(3)]
    area = row(big_ref, 6 * GROUP + 6)
    pull = spread_scale * area
    out_coef = [length[k] * grad[k] for k in range(3)]
    in_coef = back(*out_coef)
    out_coef = [pull * c for c in out_coef]
    in_coef = [pull * c for c in in_coef]
    mid_coef = -(out_coef[0] + out_coef[1] + out_coef[2] + in_coef[0] + in_coef[1] + in_coef[2])

    def first_spread(l, carry):
        w = [length[k] * dyn(big_ref, (3 + k) * GROUP + l) for k in range(3)]
        w_in = back(*w)
        total = (w[0] - w_in[0]) + (w[1] - w_in[1]) + (w[2] - w_in[2])
        at = pl.ds(pl.multiple_of(8 * l, 8), 8)
        t_ref[at, :] = dyn(big_ref, GROUP + l) - pull * total
        hist_ref[at, :] = dyn(big_ref, l)
        return carry

    lax.fori_loop(0, levels, first_spread, 0, unroll=55)

    middle = levels // 2
    c = [row(big_ref, 2 * GROUP + l) for l in range(levels)] + [jnp.zeros((8, 128), F32)]
    diag = [1.0 + c[l] + c[l + 1] for l in range(levels)]
    inverse = [None] * levels
    older, old = None, jnp.ones((8, 128), F32)
    for l in range(middle):
        new = diag[l] * old if older is None else diag[l] * old - c[l] * c[l] * older
        inverse[l] = old / new
        older, old = old, new
    older, old = None, jnp.ones((8, 128), F32)
    for l in range(levels - 1, middle, -1):
        new = diag[l] * old if older is None else diag[l] * old - c[l + 1] * c[l + 1] * older
        inverse[l] = old / new
        older, old = old, new
    m = middle
    inverse[m] = 1.0 / (
        diag[m] - c[m] * c[m] * inverse[m - 1] - c[m + 1] * c[m + 1] * inverse[m + 1]
    )
    for l in range(levels):
        inv_ref[8 * l : 8 * l + 8, :] = inverse[l]
        al_ref[8 * l : 8 * l + 8, :] = c[l] * inverse[l]
        be_ref[8 * l : 8 * l + 8, :] = c[l + 1] * inverse[l]

    def substep(n, carry):
        here = n * (levels * 8)
        there = here + levels * 8

        def source(l):
            p = hist_ref[pl.ds(pl.multiple_of(here + 8 * l, 8), 8), :]
            fore = ups(p)
            rear = back(p, p, p)
            t = row(t_ref, l) + mid_coef * p
            for k in range(3):
                t = t + (out_coef[k] * fore[k] + in_coef[k] * rear[k])
            t_ref[8 * l : 8 * l + 8, :] = t
            f_ref[8 * l : 8 * l + 8, :] = (p + t) * row(inv_ref, l)

        def put(l, value):
            hist_ref[pl.ds(pl.multiple_of(there + 8 * l, 8), 8), :] = value

        for l in range(levels):
            source(l)
        low, high = row(f_ref, 0), row(f_ref, levels - 1)
        for l in range(1, middle):
            h = levels - 1 - l
            low = row(f_ref, l) + row(al_ref, l) * low
            high = row(f_ref, h) + row(be_ref, h) * high
            f_ref[8 * l : 8 * l + 8, :] = low
            f_ref[8 * h : 8 * h + 8, :] = high
        low = high = row(f_ref, middle) + row(al_ref, middle) * low + row(be_ref, middle) * high
        put(middle, low)
        for l in range(middle - 1, -1, -1):
            h = levels - 1 - l
            low = row(f_ref, l) + row(be_ref, l) * low
            high = row(f_ref, h) + row(al_ref, h) * high
            put(l, low)
            put(h, high)
        return carry

    lax.fori_loop(0, SUBSTEPS, substep, 0, unroll=True)

    scale = [g * (1.0 / SUBSTEPS) for g in grad]
    drain = tracer_scale * area

    def finish(l, carry):
        at = pl.ds(pl.multiple_of(8 * l, 8), 8)
        total = None
        weighted = None
        for n in range(SUBSTEPS):
            p = hist_ref[pl.ds(pl.multiple_of(8 * (levels * n + l), 8), 8), :]
            total = p if total is None else total + p
            weighted = total if weighted is None else weighted + total
        out_ref[at, :] = hist_ref[pl.ds(pl.multiple_of(8 * (levels * SUBSTEPS + l), 8), 8), :]
        shifted = ups(total)
        weight_shift = ups(weighted)
        for k in range(3):
            dq_ref[pl.ds(pl.multiple_of(8 * (GROUP * k + l), 8), 8), :] = shifted[k] - total
            mean = dyn(big_ref, (3 + k) * GROUP + l) - scale[k] * (weight_shift[k] - weighted)
            flow_ref[pl.ds(pl.multiple_of(8 * (GROUP * k + l), 8), 8), :] = length[k] * jnp.maximum(mean, 0.0)
            flow_ref[pl.ds(pl.multiple_of(8 * (GROUP * (3 + k) + l), 8), 8), :] = length[k] * jnp.minimum(mean, 0.0)
        return carry

    lax.fori_loop(0, levels, finish, 0, unroll=55)

    def carry_tracers(l, carry):
        toward = [dyn(flow_ref, GROUP * k + l) for k in range(3)]
        away = [dyn(flow_ref, GROUP * (3 + k) + l) for k in range(3)]
        toward_in = back(*toward)
        away_in = back(*away)
        keep = (toward[0] - away_in[0]) + (toward[1] - away_in[1]) + (toward[2] - away_in[2])
        for s in range(species):
            tr = dyn(trc_ref, s * GROUP + l)
            beyond = ups(tr)
            before = back(tr, tr, tr)
            spread = keep * tr
            for k in range(3):
                spread = spread + (away[k] * beyond[k] - toward_in[k] * before[k])
            out_ref[pl.ds(pl.multiple_of(8 * ((s + 1) * GROUP + l), 8), 8), :] = tr - drain * spread
        return carry

    lax.fori_loop(0, levels, carry_tracers, 0, unroll=55)

    kept = (iota((1, 128), 1) & 31) - DEPTH
    kept = (kept >= 0) & (kept < SIDE)

    def folded(ref, begin, count):
        blocks = [ref[pl.ds(8 * begin + 2 + s, count, stride=8), :] for s in range(4)]
        pairs = [jnp.where(kept, blocks[s], pltpu.roll(blocks[s + 1], SIDE, 1)) for s in (0, 2)]
        return jnp.concatenate(pairs, axis=1)

    cells = pick(folded(out_ref, 0, 4 * GROUP), cell_hot_ref[...])
    newp_ref[...] = cells[0:levels]
    for s in range(species):
        newt_ref[s] = cells[(s + 1) * GROUP : (s + 1) * GROUP + levels]
    turned = jnp.zeros((GROUP, edges), F32)
    for k in range(3):
        turned = turned + pick(folded(dq_ref, GROUP * k, GROUP), edge_hot_ref[256 * k : 256 * k + 256])
    sense = meta_ref[1:2, :].astype(F32)
    newv_ref[...] = vel_ref[...] - (grad_scale * sense * flat(invd_ref)) * turned[0:levels]


def passed_along(value, axis, steps):
    count = lax.axis_size(axis)
    pairs = [(source, (source + steps) % count) for source in range(count)]
    return lax.ppermute(value, axis, pairs)


INTERPRET = False


def per_device(
    pressure, velocity, tracers, tendency, pattern, coupling, edge_length, inv_distance, inv_area,
    edge_ends, halo_ends, cell_edges, cell_signs, cell_send, edge_send,
):
    levels, edges = velocity.shape
    species = tracers.shape[0]
    stride = lax.axis_size("blk") // 16
    rows = 6 * GROUP + 8
    trows = species * GROUP
    shape = jax.ShapeDtypeStruct
    vmem = pl.BlockSpec(memory_space=pltpu.VMEM)
    inputs = (
        cell_send, edge_ends, pressure, velocity, tracers, tendency, pattern, coupling, edge_length,
        inv_distance, inv_area,
    )
    inputs = [pltpu.with_memory_space_constraint(array, pltpu.HBM) for array in inputs]
    own, trc, up, down, east, west, meta = pl.pallas_call(
        prepare,
        out_shape=(
            shape((rows, CELLS), F32), shape((trows, CELLS), F32),
            shape((rows, 128), F32), shape((rows, 128), F32), shape((rows, 128), F32), shape((rows, 128), F32),
            shape((8, edges), I32),
        ),
        in_specs=[pl.BlockSpec(memory_space=pltpu.HBM)] * 11,
        out_specs=(vmem,) * 7,
        scratch_shapes=[
            pltpu.VMEM((3 * GROUP + 8 + trows, CELLS), F32), pltpu.VMEM((GROUP + 8, edges), F32),
            pltpu.SMEM(cell_send.shape, I32),
        ] + [pltpu.VMEM(array.shape, array.dtype) for array in inputs[1:]] + [pltpu.SemaphoreType.DMA((11,))],
        compiler_params=pltpu.CompilerParams(vmem_limit_bytes=40 * 2**20),
        interpret=INTERPRET,
        name="prepare",
    )(*inputs)
    south = passed_along(up, "blk", stride)
    north = passed_along(down, "blk", -stride)
    half = shape((rows - trows, 384), F32)
    to_east, to_west = pl.pallas_call(
        pack,
        out_shape=(half, half),
        in_specs=[vmem] * 4,
        out_specs=(vmem,) * 2,
        compiler_params=pltpu.CompilerParams(vmem_limit_bytes=40 * 2**20),
        interpret=INTERPRET,
        name="pack",
    )(east, west, south, north)
    from_west = passed_along(to_east, "blk", 1)
    from_east = passed_along(to_west, "blk", -1)
    core, tcore, cell_hot, edge_hot = pl.pallas_call(
        settle,
        out_shape=(
            shape((rows, 512), F32), shape((trows, 512), F32), shape((CELLS, CELLS), BF16),
            shape((3 * CELLS, edges), BF16),
        ),
        in_specs=[vmem] * 5,
        out_specs=(vmem,) * 4,
        compiler_params=pltpu.CompilerParams(vmem_limit_bytes=30 * 2**20),
        interpret=INTERPRET,
        name="settle",
    )(own, trc, south, north, meta)
    block = pltpu.VMEM((levels * 8, 128), F32)
    return pl.pallas_call(
        advance,
        out_shape=(
            shape((levels, CELLS), F32), shape((levels, edges), F32), shape((species, levels, CELLS), F32),
        ),
        in_specs=[vmem] * 9,
        out_specs=(vmem,) * 3,
        scratch_shapes=[
            pltpu.VMEM((rows * 8, 128), F32), pltpu.VMEM((trows * 8, 128), F32),
            pltpu.VMEM(((SUBSTEPS + 1) * levels * 8, 128), F32),
            block, block, block, block, block,
            pltpu.VMEM((4 * GROUP * 8, 128), F32), pltpu.VMEM((3 * GROUP * 8, 128), F32),
            pltpu.VMEM((6 * GROUP * 8, 128), F32),
        ],
        compiler_params=pltpu.CompilerParams(vmem_limit_bytes=40 * 2**20),
        interpret=INTERPRET,
        name="advance",
    )(core, tcore, from_west, from_east, cell_hot, edge_hot, meta, velocity, inv_distance)


def solution(mesh):
    both = ("member", "blk")
    in_specs = (
        P(None, both), P(None, both), P(None, None, both), P(None, both), P(both),
        P(None, "blk"), P("blk"), P("blk"), P("blk"),
        P(None, "blk"), P(None, "blk"), P(None, "blk"), P(None, "blk"), P(None, "blk"), P(None, "blk"),
    )
    out_specs = (P(None, both), P(None, both), P(None, None, both))
    return jax.shard_map(
        per_device, mesh=mesh, in_specs=in_specs, out_specs=out_specs, check_vma=False
    )
```

```python
import jax
import jax.numpy as jnp
from jax import lax
from jax.experimental import pallas as pl
from jax.experimental.pallas import tpu as pltpu
from jax.sharding import PartitionSpec as P


SUBSTEPS = 6
grad_scale = 0.25
spread_scale = 0.25
force_scale = 0.5
tracer_scale = 0.05

SIDE = 16
CELLS = SIDE * SIDE
DEPTH = SUBSTEPS
COL = 32
PAD_A = 8
GROUP = 56
F32 = jnp.float32
BF16 = jnp.bfloat16
I32 = jnp.int32


def iota(shape, dim):
    return lax.broadcasted_iota(I32, shape, dim)


def one_hot(row, count):
    return jnp.where(iota((count, row.shape[1]), 0) == row, 1.0, 0.0).astype(BF16)


def halves(x):
    hi = x.astype(BF16)
    return hi, (x - hi.astype(F32)).astype(BF16)


def dot(x, y):
    return lax.dot_general(x, y, (((1,), (0,)), ((), ())), preferred_element_type=F32)


def dot_t(x, y):
    return lax.dot_general(x, y, (((1,), (1,)), ((), ())), preferred_element_type=F32)


def pick(x, table):
    hi, lo = halves(x)
    return dot(hi, table) + dot(lo, table)


def pick_t(x, table):
    hi, lo = halves(x)
    return dot_t(hi, table) + dot_t(lo, table)


def rows8(*rows):
    width = rows[0].shape[1]
    at = iota((8, width), 0)
    out = jnp.zeros((8, width), F32)
    for number, row in enumerate(rows):
        out = jnp.where(at == number, row, out)
    return out


def odd_patch():
    return (lax.axis_index("blk") & 1) == 1


def odd_line():
    return ((lax.axis_index("blk") // SIDE) & 1) == 1


def either(flag, x, y):
    return jnp.where(jnp.broadcast_to(flag, x.shape), x, y)


def flat(ref):
    return ref[...].reshape(1, ref.shape[0])


def sixth(j):
    return (j * 43) >> 8


def prepare(*refs):
    sources, rest = refs[:11], refs[11:]
    own_ref, trcl_ref, up_ref, dn_ref, east_ref, west_ref, meta_ref, x_ref, v_ref = rest[:9]
    send_ref, ends_ref, p_ref, vel_ref, trc_ref, tend_ref, pat_ref, coup_ref, len_ref, invd_ref, ia_ref = rest[9:20]
    arrived = rest[20]
    copies = [pltpu.make_async_copy(src, dst, arrived.at[n]) for n, (src, dst) in enumerate(zip(sources, rest[9:20]))]
    for copy in copies:
        copy.start()
    copies[0].wait()
    copies[1].wait()
    levels = p_ref.shape[0]
    edges = vel_ref.shape[1]
    start = ends_ref[0:1, :]
    end = ends_ref[1:2, :]
    start_hot = one_hot(start, CELLS)
    end_hot = one_hot(end, CELLS)
    joined = dot_t(
        jnp.concatenate([start_hot, end_hot], axis=1), jnp.concatenate([end_hot, start_hot], axis=1)
    )
    same = iota((CELLS, CELLS), 0) == iota((CELLS, CELLS), 1)
    step1 = jnp.where(same, 1.0, jnp.minimum(1.0, joined)).astype(BF16)
    step2 = jnp.minimum(1.0, dot(step1, step1)).astype(BF16)
    step4 = jnp.minimum(1.0, dot(step2, step2)).astype(BF16)
    cell = iota((1, CELLS), 1)
    seeds = []
    for side in (1, 0, 3, 2):
        hit = cell == send_ref[side, 0]
        for s in range(1, SIDE):
            hit = hit | (cell == send_ref[side, s])
        seeds.append(jnp.where(hit, 1.0, 0.0))
    reached = rows8(*seeds)
    for step in (step1, step2, step4):
        wider = jnp.minimum(1.0, dot(reached.astype(BF16), step))
        reached = jnp.concatenate([reached, wider], axis=0)
    far = jnp.zeros((8, CELLS), F32)
    for n in range(SIDE // 2):
        far = far + (1.0 - reached[8 * n : 8 * n + 8])
    half = SIDE // 2
    a = jnp.where(far[0:1] < half, far[0:1], SIDE - 1.0 - far[1:2])
    b = jnp.where(far[2:3] < half, far[2:3], SIDE - 1.0 - far[3:4])
    place = (a * SIDE + b).astype(I32)
    corners = rows8(a, b).astype(BF16)
    at_start = dot(corners, start_hot)
    at_end = dot(corners, end_hot)
    a_s, b_s = at_start[0:1], at_start[1:2]
    a_e, b_e = at_end[0:1], at_end[1:2]
    rim_hot = one_hot(end - CELLS, 6 * SIDE)
    met = dot_t(rows8(b_s, jnp.ones_like(b_s)).astype(BF16), rim_hot)
    rim_b = jnp.where(met[1:2] > 1.5, (met[0:1] - 1.0) * 0.5, met[0:1])
    rim_b = dot(rows8(rim_b).astype(BF16), rim_hot)[0:1]
    outside = end >= CELLS
    peer = (end - CELLS) >> 4
    zero = jnp.zeros_like(end)
    direction_out = jnp.where(
        peer == 3, zero + 1, jnp.where(peer == 1, jnp.where(jnp.abs(b_s - rim_b) < 0.5, zero, zero + 2), zero + 2)
    )
    da = a_e - a_s
    db = b_e - b_s
    direction_in = jnp.where(jnp.abs(db) < 0.5, zero, jnp.where(jnp.abs(da) < 0.5, zero + 1, zero + 2))
    onward = outside | (da > 0.5) | ((jnp.abs(da) < 0.5) & (db > 0.5))
    direction = jnp.where(outside, direction_out, direction_in)
    sense = jnp.where(onward, 1.0, -1.0)
    anchor = jnp.where(onward, a_s * SIDE + b_s, a_e * SIDE + b_e).astype(I32)
    spot = direction * CELLS + anchor
    at8 = iota((8, edges), 0)
    meta = jnp.where(at8 == 0, spot, jnp.where(at8 == 1, sense.astype(I32), zero))
    meta_ref[...] = meta
    meta_ref[2:3, 0:CELLS] = place
    for copy in copies[2:]:
        copy.wait()
    x_ref[...] = jnp.zeros(x_ref.shape, F32)
    height = iota((levels, 1), 0).astype(F32)
    taper = jnp.minimum(1.0, (levels - 1.0 - height) / (0.25 * levels))
    x_ref[0:levels] = p_ref[...]
    x_ref[GROUP : GROUP + levels] = force_scale * (1.0 + flat(pat_ref) * taper) * tend_ref[...]
    x_ref[2 * GROUP : 2 * GROUP + levels] = coup_ref[...]
    x_ref[3 * GROUP : 3 * GROUP + 1] = flat(ia_ref)
    first = 3 * GROUP + 8
    for n in range(trc_ref.shape[0]):
        x_ref[first + n * GROUP : first + n * GROUP + levels] = trc_ref[n]
    place_hot = one_hot(place, CELLS)
    moved = pick_t(x_ref[...], place_hot)
    own_ref[0 : 3 * GROUP] = moved[0 : 3 * GROUP]
    trcl_ref[...] = moved[first:]
    v_ref[...] = jnp.zeros(v_ref.shape, F32)
    v_ref[0:levels] = vel_ref[...] * sense
    v_ref[GROUP : GROUP + 1] = flat(len_ref)
    v_ref[GROUP + 1 : GROUP + 2] = flat(invd_ref)
    v_hi, v_lo = halves(v_ref[...])
    lengths, distances = [], []
    for k in range(3):
        spot_hot = one_hot(spot - k * CELLS, CELLS)
        got = dot_t(v_hi, spot_hot) + dot_t(v_lo, spot_hot)
        own_ref[(3 + k) * GROUP : (4 + k) * GROUP] = got[0:GROUP]
        lengths.append(got[GROUP : GROUP + 1])
        distances.append(got[GROUP + 1 : GROUP + 2])
    own_ref[6 * GROUP : 6 * GROUP + 8] = rows8(*lengths, *distances, moved[3 * GROUP : 3 * GROUP + 1])
    column = iota((1, 512), 1)
    part = column >> 7
    part = either(odd_line(), jnp.where(part < 2, 1 - part, part), part)
    j = column & 127
    sa = sixth(j)
    sb = j - sa * 6
    strip = jnp.where(
        part == 0, sa * SIDE + SIDE - DEPTH + sb,
        jnp.where(part == 1, sa * SIDE + sb, jnp.where(part == 2, j + CELLS - DEPTH * SIDE, j)),
    )
    strip = jnp.where(j < DEPTH * SIDE, strip, -1)
    t = j - DEPTH * SIDE
    rim = jnp.where(
        part == 0, t * SIDE + SIDE - 1, jnp.where(part == 1, t * SIDE, jnp.where(part == 2, t + CELLS - SIDE, t))
    )
    rim = jnp.where((t >= 0) & (t < SIDE), rim, -1)
    strips = pick(own_ref[...], one_hot(strip, CELLS))
    rims = pick(trcl_ref[...], one_hot(rim, CELLS))
    top = strips[0 : rims.shape[0]] + rims
    rest = strips[rims.shape[0] :]
    for number, ref in enumerate((up_ref, dn_ref, east_ref, west_ref)):
        ref[0 : rims.shape[0]] = top[:, 128 * number : 128 * number + 128]
        ref[rims.shape[0] :] = rest[:, 128 * number : 128 * number + 128]


def pack(east_ref, west_ref, pair_ref, cross_ref, to_pair_ref, to_cross_ref):
    rows = east_ref.shape[0]
    split = rows - to_pair_ref.shape[0]
    flag = odd_line()
    south = either(flag, pair_ref[...], cross_ref[...])
    north = either(flag, cross_ref[...], pair_ref[...])
    cut = DEPTH * DEPTH
    wide = DEPTH * SIDE
    rim = wide + SIDE
    for out in (to_pair_ref, to_cross_ref):
        out[split:, 0:256] = jnp.zeros((out.shape[0] - split, 256), F32)
    for begin, end, at in ((0, split, 0), (split, rows, 192)):
        count = end - begin
        lines = []
        for part, body, corner in ((east_ref, wide - cut, rim - 1), (west_ref, 0, wide)):
            lines.append(jnp.concatenate([
                part[begin:end, 0:rim], south[begin:end, body : body + cut], north[begin:end, body : body + cut],
                south[begin:end, corner : corner + 1], north[begin:end, corner : corner + 1],
                jnp.zeros((count, 6), F32),
            ], axis=1))
        flag = odd_patch()
        to_pair_ref[0:count, at : at + 192] = either(flag, lines[1], lines[0])
        to_cross_ref[0:count, at : at + 192] = either(flag, lines[0], lines[1])


def settle(own_ref, trcl_ref, pair_ref, cross_ref, meta_ref, core_ref, tcore_ref, cell_hot_ref, edge_hot_ref):
    trows = trcl_ref.shape[0]
    q = iota((1, 512), 1)
    qa = q >> 5
    qb = (q & 31) - DEPTH
    inside = (qb >= 0) & (qb < SIDE)
    below = (qb >= -DEPTH) & (qb < 0)
    above = (qb >= SIDE) & (qb < SIDE + DEPTH)
    src = jnp.where(inside, qa * SIDE + qb, -1)
    rsrc = jnp.where(below, qa * DEPTH + qb + DEPTH, jnp.where(above, 128 + qa * DEPTH + qb - SIDE, -1))
    tsrc = jnp.where(qb == -1, 96 + qa, jnp.where(qb == SIDE, 128 + 96 + qa, -1))
    flag = odd_line()
    south = either(flag, pair_ref[...], cross_ref[...])
    north = either(flag, cross_ref[...], pair_ref[...])
    sn_hi, sn_lo = halves(jnp.concatenate([south, north], axis=1))
    own_hot = one_hot(src, 256)
    rim_hot = one_hot(rsrc, 256)
    core_ref[...] = pick(own_ref[...], own_hot) + (dot(sn_hi, rim_hot) + dot(sn_lo, rim_hot))
    rim_hot = one_hot(tsrc, 256)
    tcore_ref[...] = pick(trcl_ref[...], own_hot) + (dot(sn_hi[0:trows], rim_hot) + dot(sn_lo[0:trows], rim_hot))

    def lane_of(place):
        column = place >> 4
        at = ((column & 3) << 5) + (place & 15) + DEPTH + ((column >> 2) & 1) * SIDE
        return ((column >> 3) << 7) + (at & 127)

    cell_hot_ref[...] = one_hot(lane_of(meta_ref[2:3, 0:CELLS]), 256)
    spot = meta_ref[0:1, :]
    for k in range(3):
        place = spot - k * CELLS
        at = jnp.where((place >= 0) & (place < CELLS), lane_of(place & (CELLS - 1)), -1)
        edge_hot_ref[256 * k : 256 * k + 256] = one_hot(at, 256)


def advance(
    core_ref, tcore_ref, pair_ref, cross_ref, cell_hot_ref, edge_hot_ref, meta_ref, vel_ref, invd_ref,
    newp_ref, newv_ref, newt_ref,
    big_ref, trc_ref, hist_ref, t_ref, f_ref, inv_ref, al_ref, be_ref, out_ref, dq_ref, flow_ref,
):
    levels = newp_ref.shape[0]
    species = newt_ref.shape[0]
    edges = newv_ref.shape[1]
    rows = core_ref.shape[0]
    trows = tcore_ref.shape[0]
    for s in range(4):
        big_ref[pl.ds(2 + s, rows, stride=8), :] = core_ref[:, 128 * s : 128 * s + 128]
        trc_ref[pl.ds(2 + s, trows, stride=8), :] = tcore_ref[:, 128 * s : 128 * s + 128]
    q = iota((1, 256), 1)
    qb = (q & 31) - DEPTH
    inside = (qb >= 0) & (qb < SIDE)
    below = (qb >= -DEPTH) & (qb < 0)
    above = (qb >= SIDE) & (qb < SIDE + DEPTH)
    flag = odd_patch()
    west = either(flag, pair_ref[...], cross_ref[...])
    east = either(flag, cross_ref[...], pair_ref[...])
    for side, value in ((0, west), (6, east)):
        qa = (q >> 5) - (PAD_A - DEPTH if side == 0 else 0)
        src = jnp.where(
            inside, qa * SIDE + qb,
            jnp.where(below, 112 + qa * DEPTH + qb + DEPTH, jnp.where(above, 148 + qa * DEPTH + qb - SIDE, -1)),
        )
        src = jnp.where((qa >= 0) & (qa < DEPTH), src, -1)
        near = DEPTH - 1 if side == 0 else 0
        tsrc = jnp.where(
            inside, 96 + qb, jnp.where(qb == -1, 184, jnp.where(qb == SIDE, 185, -1))
        )
        tsrc = jnp.where(qa == near, tsrc, -1)
        hi, lo = halves(value)
        hot = one_hot(src, 256)
        thot = one_hot(tsrc, 256)
        late_hot = one_hot(jnp.where(src >= 0, src + 64, -1), 256)
        flank = dot(hi[0:trows, 0:256], hot) + dot(lo[0:trows, 0:256], hot)
        late = dot(hi[:, 128:384], late_hot) + dot(lo[:, 128:384], late_hot)
        tflank = dot(hi[0:trows, 0:256], thot) + dot(lo[0:trows, 0:256], thot)
        for s in range(2):
            cut = slice(128 * s, 128 * s + 128)
            big_ref[pl.ds(side + s, trows, stride=8), :] = flank[:, cut]
            big_ref[pl.ds(8 * trows + side + s, rows - trows, stride=8), :] = late[:, cut]
            trc_ref[pl.ds(side + s, trows, stride=8), :] = tflank[:, cut]

    lane = iota((8, 128), 1)

    def ahead(x, step):
        y = pltpu.roll(x, 128 - step, 1)
        return jnp.where(lane >= 128 - step, pltpu.roll(y, 7, 0), y)

    def behind(x, step):
        y = pltpu.roll(x, step, 1)
        return jnp.where(lane < step, pltpu.roll(y, 1, 0), y)

    def ups(x):
        return ahead(x, COL), pltpu.roll(x, 127, 1), ahead(x, COL - 1)

    def back(x0, x1, x2):
        return behind(x0, COL), pltpu.roll(x1, 1, 1), behind(x2, COL - 1)

    def row(ref, number):
        return ref[8 * number : 8 * number + 8, :]

    def dyn(ref, number):
        return ref[pl.ds(pl.multiple_of(8 * number, 8), 8), :]

    length = [row(big_ref, 6 * GROUP + k) for k in range(3)]
    grad = [grad_scale * row(big_ref, 6 * GROUP + 3 + k) for k in range(3)]
    area = row(big_ref, 6 * GROUP + 6)
    pull = spread_scale * area
    out_coef = [length[k] * grad[k] for k in range(3)]
    in_coef = back(*out_coef)
    out_coef = [pull * c for c in out_coef]
    in_coef = [pull * c for c in in_coef]
    mid_coef = -(out_coef[0] + out_coef[1] + out_coef[2] + in_coef[0] + in_coef[1] + in_coef[2])

    def first_spread(l, carry):
        w = [length[k] * dyn(big_ref, (3 + k) * GROUP + l) for k in range(3)]
        w_in = back(*w)
        total = (w[0] - w_in[0]) + (w[1] - w_in[1]) + (w[2] - w_in[2])
        at = pl.ds(pl.multiple_of(8 * l, 8), 8)
        t_ref[at, :] = dyn(big_ref, GROUP + l) - pull * total
        hist_ref[at, :] = dyn(big_ref, l)
        return carry

    lax.fori_loop(0, levels, first_spread, 0, unroll=55)

    middle = levels // 2
    c = [row(big_ref, 2 * GROUP + l) for l in range(levels)] + [jnp.zeros((8, 128), F32)]
    diag = [1.0 + c[l] + c[l + 1] for l in range(levels)]
    inverse = [None] * levels
    older, old = None, jnp.ones((8, 128), F32)
    for l in range(middle):
        new = diag[l] * old if older is None else diag[l] * old - c[l] * c[l] * older
        inverse[l] = old / new
        older, old = old, new
    older, old = None, jnp.ones((8, 128), F32)
    for l in range(levels - 1, middle, -1):
        new = diag[l] * old if older is None else diag[l] * old - c[l + 1] * c[l + 1] * older
        inverse[l] = old / new
        older, old = old, new
    m = middle
    inverse[m] = 1.0 / (
        diag[m] - c[m] * c[m] * inverse[m - 1] - c[m + 1] * c[m + 1] * inverse[m + 1]
    )
    for l in range(levels):
        inv_ref[8 * l : 8 * l + 8, :] = inverse[l]
        al_ref[8 * l : 8 * l + 8, :] = c[l] * inverse[l]
        be_ref[8 * l : 8 * l + 8, :] = c[l + 1] * inverse[l]

    def substep(n, carry):
        here = n * (levels * 8)
        there = here + levels * 8

        def source(l):
            p = hist_ref[pl.ds(pl.multiple_of(here + 8 * l, 8), 8), :]
            fore = ups(p)
            rear = back(p, p, p)
            t = row(t_ref, l) + mid_coef * p
            for k in range(3):
                t = t + (out_coef[k] * fore[k] + in_coef[k] * rear[k])
            t_ref[8 * l : 8 * l + 8, :] = t
            f_ref[8 * l : 8 * l + 8, :] = (p + t) * row(inv_ref, l)

        def put(l, value):
            hist_ref[pl.ds(pl.multiple_of(there + 8 * l, 8), 8), :] = value

        for l in range(levels):
            source(l)
        low, high = row(f_ref, 0), row(f_ref, levels - 1)
        for l in range(1, middle):
            h = levels - 1 - l
            low = row(f_ref, l) + row(al_ref, l) * low
            high = row(f_ref, h) + row(be_ref, h) * high
            f_ref[8 * l : 8 * l + 8, :] = low
            f_ref[8 * h : 8 * h + 8, :] = high
        low = high = row(f_ref, middle) + row(al_ref, middle) * low + row(be_ref, middle) * high
        put(middle, low)
        for l in range(middle - 1, -1, -1):
            h = levels - 1 - l
            low = row(f_ref, l) + row(be_ref, l) * low
            high = row(f_ref, h) + row(al_ref, h) * high
            put(l, low)
            put(h, high)
        return carry

    lax.fori_loop(0, SUBSTEPS, substep, 0, unroll=True)

    scale = [g * (1.0 / SUBSTEPS) for g in grad]
    drain = tracer_scale * area

    def finish(l, carry):
        at = pl.ds(pl.multiple_of(8 * l, 8), 8)
        total = None
        weighted = None
        for n in range(SUBSTEPS):
            p = hist_ref[pl.ds(pl.multiple_of(8 * (levels * n + l), 8), 8), :]
            total = p if total is None else total + p
            weighted = total if weighted is None else weighted + total
        out_ref[at, :] = hist_ref[pl.ds(pl.multiple_of(8 * (levels * SUBSTEPS + l), 8), 8), :]
        shifted = ups(total)
        weight_shift = ups(weighted)
        for k in range(3):
            dq_ref[pl.ds(pl.multiple_of(8 * (GROUP * k + l), 8), 8), :] = shifted[k] - total
            mean = dyn(big_ref, (3 + k) * GROUP + l) - scale[k] * (weight_shift[k] - weighted)
            flow_ref[pl.ds(pl.multiple_of(8 * (GROUP * k + l), 8), 8), :] = length[k] * jnp.maximum(mean, 0.0)
            flow_ref[pl.ds(pl.multiple_of(8 * (GROUP * (3 + k) + l), 8), 8), :] = length[k] * jnp.minimum(mean, 0.0)
        return carry

    lax.fori_loop(0, levels, finish, 0, unroll=55)

    def carry_tracers(l, carry):
        toward = [dyn(flow_ref, GROUP * k + l) for k in range(3)]
        away = [dyn(flow_ref, GROUP * (3 + k) + l) for k in range(3)]
        toward_in = back(*toward)
        away_in = back(*away)
        keep = (toward[0] - away_in[0]) + (toward[1] - away_in[1]) + (toward[2] - away_in[2])
        for s in range(species):
            tr = dyn(trc_ref, s * GROUP + l)
            beyond = ups(tr)
            before = back(tr, tr, tr)
            spread = keep * tr
            for k in range(3):
                spread = spread + (away[k] * beyond[k] - toward_in[k] * before[k])
            out_ref[pl.ds(pl.multiple_of(8 * ((s + 1) * GROUP + l), 8), 8), :] = tr - drain * spread
        return carry

    lax.fori_loop(0, levels, carry_tracers, 0, unroll=55)

    kept = (iota((1, 128), 1) & 31) - DEPTH
    kept = (kept >= 0) & (kept < SIDE)

    def folded(ref, begin, count):
        blocks = [ref[pl.ds(8 * begin + 2 + s, count, stride=8), :] for s in range(4)]
        pairs = [jnp.where(kept, blocks[s], pltpu.roll(blocks[s + 1], SIDE, 1)) for s in (0, 2)]
        return jnp.concatenate(pairs, axis=1)

    cells = pick(folded(out_ref, 0, 4 * GROUP), cell_hot_ref[...])
    newp_ref[...] = cells[0:levels]
    for s in range(species):
        newt_ref[s] = cells[(s + 1) * GROUP : (s + 1) * GROUP + levels]
    turned = jnp.zeros((GROUP, edges), F32)
    for k in range(3):
        turned = turned + pick(folded(dq_ref, GROUP * k, GROUP), edge_hot_ref[256 * k : 256 * k + 256])
    sense = meta_ref[1:2, :].astype(F32)
    newv_ref[...] = vel_ref[...] - (grad_scale * sense * flat(invd_ref)) * turned[0:levels]


def swapped(value, axis, steps, first):
    count = lax.axis_size(axis)
    pairs = []
    for source in range(count):
        onward = (source // steps) % 2 == first
        pairs.append((source, (source + (steps if onward else -steps)) % count))
    return lax.ppermute(value, axis, pairs)


INTERPRET = False


def per_device(
    pressure, velocity, tracers, tendency, pattern, coupling, edge_length, inv_distance, inv_area,
    edge_ends, halo_ends, cell_edges, cell_signs, cell_send, edge_send,
):
    levels, edges = velocity.shape
    species = tracers.shape[0]
    stride = lax.axis_size("blk") // 16
    rows = 6 * GROUP + 8
    trows = species * GROUP
    shape = jax.ShapeDtypeStruct
    vmem = pl.BlockSpec(memory_space=pltpu.VMEM)
    inputs = (
        cell_send, edge_ends, pressure, velocity, tracers, tendency, pattern, coupling, edge_length,
        inv_distance, inv_area,
    )
    inputs = [pltpu.with_memory_space_constraint(array, pltpu.HBM) for array in inputs]
    own, trc, up, down, east, west, meta = pl.pallas_call(
        prepare,
        out_shape=(
            shape((rows, CELLS), F32), shape((trows, CELLS), F32),
            shape((rows, 128), F32), shape((rows, 128), F32), shape((rows, 128), F32), shape((rows, 128), F32),
            shape((8, edges), I32),
        ),
        in_specs=[pl.BlockSpec(memory_space=pltpu.HBM)] * 11,
        out_specs=(vmem,) * 7,
        scratch_shapes=[
            pltpu.VMEM((3 * GROUP + 8 + trows, CELLS), F32), pltpu.VMEM((GROUP + 8, edges), F32),
            pltpu.SMEM(cell_send.shape, I32),
        ] + [pltpu.VMEM(array.shape, array.dtype) for array in inputs[1:]] + [pltpu.SemaphoreType.DMA((11,))],
        compiler_params=pltpu.CompilerParams(vmem_limit_bytes=40 * 2**20),
        interpret=INTERPRET,
        name="prepare",
    )(*inputs)
    line_pair = swapped(up, "blk", stride, 0)
    line_cross = swapped(down, "blk", stride, 1)
    half = shape((rows - trows, 384), F32)
    to_pair, to_cross = pl.pallas_call(
        pack,
        out_shape=(half, half),
        in_specs=[vmem] * 4,
        out_specs=(vmem,) * 2,
        compiler_params=pltpu.CompilerParams(vmem_limit_bytes=40 * 2**20),
        interpret=INTERPRET,
        name="pack",
    )(east, west, line_pair, line_cross)
    from_cross = swapped(to_cross, "blk", 1, 1)
    from_pair = swapped(to_pair, "blk", 1, 0)
    core, tcore, cell_hot, edge_hot = pl.pallas_call(
        settle,
        out_shape=(
            shape((rows, 512), F32), shape((trows, 512), F32), shape((CELLS, CELLS), BF16),
            shape((3 * CELLS, edges), BF16),
        ),
        in_specs=[vmem] * 5,
        out_specs=(vmem,) * 4,
        compiler_params=pltpu.CompilerParams(vmem_limit_bytes=30 * 2**20),
        interpret=INTERPRET,
        name="settle",
    )(own, trc, line_pair, line_cross, meta)
    block = pltpu.VMEM((levels * 8, 128), F32)
    return pl.pallas_call(
        advance,
        out_shape=(
            shape((levels, CELLS), F32), shape((levels, edges), F32), shape((species, levels, CELLS), F32),
        ),
        in_specs=[vmem] * 9,
        out_specs=(vmem,) * 3,
        scratch_shapes=[
            pltpu.VMEM((rows * 8, 128), F32), pltpu.VMEM((trows * 8, 128), F32),
            pltpu.VMEM(((SUBSTEPS + 1) * levels * 8, 128), F32),
            block, block, block, block, block,
            pltpu.VMEM((4 * GROUP * 8, 128), F32), pltpu.VMEM((3 * GROUP * 8, 128), F32),
            pltpu.VMEM((6 * GROUP * 8, 128), F32),
        ],
        compiler_params=pltpu.CompilerParams(vmem_limit_bytes=40 * 2**20),
        interpret=INTERPRET,
        name="advance",
    )(core, tcore, from_pair, from_cross, cell_hot, edge_hot, meta, velocity, inv_distance)


def solution(mesh):
    both = ("member", "blk")
    in_specs = (
        P(None, both), P(None, both), P(None, None, both), P(None, both), P(both),
        P(None, "blk"), P("blk"), P("blk"), P("blk"),
        P(None, "blk"), P(None, "blk"), P(None, "blk"), P(None, "blk"), P(None, "blk"), P(None, "blk"),
    )
    out_specs = (P(None, both), P(None, both), P(None, None, both))
    return jax.shard_map(
        per_device, mesh=mesh, in_specs=in_specs, out_specs=out_specs, check_vma=False
    )
```
